32 devices in a mesh: rep: 1 (over z), dp: 32 (over x, y, core).
Axes of the slice: x: 4, y: 4, z: 1, core: 2. Of those that a mesh axis runs over, the one named last changes fastest.
The devices are a block of a 4x4x8 slice.
Arguments:
- x: bfloat16 [32, 2048, 896], P(('rep', 'dp'))
- dy: bfloat16 [32, 2048, 896], P(('rep', 'dp'))
- w_gate: bfloat16 [2, 896, 2304], P(None, 'dp')
- w_up: bfloat16 [2, 896, 2304], P(None, 'dp')
- w_down: bfloat16 [2, 2304, 896], P(None, 'dp')
Outputs:
- output 1: bfloat16 [32, 2048, 896], P(('rep', 'dp'))
- output 2: bfloat16 [2, 896, 2304], P('rep', 'dp')
- output 3: bfloat16 [2, 896, 2304], P('rep', 'dp')
- output 4: bfloat16 [2, 2304, 896], P('rep', 'dp')
All inputs are finite; a program needn't handle non-finite values.
Results may differ from the reference program's by a relative error of at most 0.018.
Values are sent between devices in bfloat16 or wider.
A program may use at most 768 MiB of HBM per device.

```python
import jax
import jax.numpy as jnp
from jax import lax

SEQUENCES = 32
TOKENS = 2048
D = 896
FF = 2304
LAYERS = 2
NAMES = ("w_gate", "w_up", "w_down")
SHAPES = {"w_gate": (LAYERS, D, FF), "w_up": (LAYERS, D, FF), "w_down": (LAYERS, FF, D)}


def bump(key, n, height):
    away = (jnp.arange(n, dtype=jnp.int32) - jax.random.randint(key, (), 0, n, jnp.int32)) % n
    return jnp.where(away < n // 8, height, 1.0)


def together(key, own, strength):
    shared = jax.random.normal(key, own.shape[1:], jnp.float32)
    return (own + strength * shared) * lax.rsqrt(1 + strength * strength)


def setup_inputs(seed: int = 0, part: int = 0) -> dict:
    kx, kdy, ka, kb, kz, kf, kh, kl, *kw = jax.random.split(jax.random.key(seed), 8 + len(NAMES))
    kx, kdy, ka, kb = (jax.random.fold_in(k, part) for k in (kx, kdy, ka, kb))
    shape = (SEQUENCES, TOKENS, D)
    much_x, much_dy = jax.random.uniform(kz, (2,), jnp.float32, 0.0, 1.0)
    layers = 2.0 ** jax.random.uniform(kl, (LAYERS, 1, 1), jnp.float32, -1.0, 1.0)
    x = together(ka, jax.random.normal(kx, shape, jnp.float32), much_x) * bump(kf, D, 4.0)
    dy = together(kb, jax.random.normal(kdy, shape, jnp.float32), much_dy)
    drawn = {"x": x.astype(jnp.bfloat16), "dy": (dy * (SEQUENCES * TOKENS) ** -0.5).astype(jnp.bfloat16)}
    for key, name in zip(kw, NAMES, strict=True):
        w = jax.random.normal(key, SHAPES[name], jnp.float32) * SHAPES[name][1] ** -0.5
        drawn[name] = (w * {"w_gate": 1.0, "w_up": bump(kh, FF, 4.0), "w_down": layers}[name]).astype(jnp.bfloat16)
    return drawn


def matmul(a, w):
    return jnp.dot(a, w, preferred_element_type=jnp.float32).astype(jnp.bfloat16)


def normed(h):
    wide = h.astype(jnp.float32)
    scale = lax.rsqrt(jnp.mean(wide**2, -1, keepdims=True) + 1e-6)
    return (wide * scale).astype(jnp.bfloat16)


def layer(h, w):
    a = normed(h)
    gate = jnp.dot(a, w["w_gate"], preferred_element_type=jnp.float32)
    up = jnp.dot(a, w["w_up"], preferred_element_type=jnp.float32)
    return h + matmul((jax.nn.silu(gate) * up).astype(jnp.bfloat16), w["w_down"])


def stack(weights, h):
    return lax.scan(lambda h, w: (layer(h, w), None), h, weights)[0]


def reference(x, dy, w_gate, w_up, w_down):
    weights = dict(zip(NAMES, (w_gate, w_up, w_down), strict=True))

    def take(so_far, sequence):
        h, by_y = sequence
        _, back = jax.vjp(stack, weights, h)
        by_weights, by_h = back(by_y)
        return jax.tree.map(lambda total, term: total + term.astype(jnp.float32), so_far, by_weights), by_h

    none_yet = {name: jnp.zeros(w.shape, jnp.float32) for name, w in weights.items()}
    by_weights, by_x = lax.scan(take, none_yet, (x, dy))
    return (by_x, *(by_weights[name].astype(jnp.bfloat16) for name in NAMES))
```

```python
import functools
import math
import jax
import jax.numpy as jnp
from jax import lax
from jax.experimental import pallas as pl
from jax.experimental.pallas import tpu as pltpu
from jax.sharding import PartitionSpec as P

MESH = pl.DeviceIdType.MESH
F32, BF16 = jnp.float32, jnp.bfloat16
ALL = slice(None)


def halves(n):
    first = (n // 128 + 1) // 2 * 128
    return (0, first), (first, n - first)


class Place:
    def __init__(self, n):
        self.side = math.isqrt(n // 2)
        me = lax.axis_index("dp")
        chip = me // 2
        self.c = me % 2
        self.xy = (chip // self.side, chip % self.side)
        self.partner = {"dp": chip * 2 + 1 - self.c}

    def hop(self, axis, by):
        xy = list(self.xy)
        xy[axis] = lax.rem(xy[axis] + by + self.side, self.side)
        return {"dp": (xy[0] * self.side + xy[1]) * 2 + self.c}

    def at(self, axis, by):
        return lax.rem(self.xy[axis] + by + self.side, self.side)

    def greet(self):
        barrier = pltpu.get_barrier_semaphore()
        others = [self.partner] + [self.hop(a, d) for a in (0, 1) for d in (1, -1)]
        for other in others:
            pl.semaphore_signal(barrier, inc=1, device_id=other, device_id_type=MESH)
        pl.semaphore_wait(barrier, len(others))


class Sems:
    def __init__(self, send, recv):
        self.send, self.recv, self.used, self.started = send, recv, 0, []

    def copy(self, src, dst, to):
        k = self.used
        self.used += 1
        made = pltpu.make_async_remote_copy(
            src_ref=src, dst_ref=dst, send_sem=self.send.at[k], recv_sem=self.recv.at[k], device_id=to, device_id_type=MESH
        )
        made.start()
        self.started.append(made)
        return made

    def finish(self):
        for made in self.started:
            made.wait_send()


def order(axis, a, b):
    return (a, b) if axis == 0 else (b, a)


class Gather:
    def __init__(self, place, sems, view, other_view, own, axis, lanes):
        self.place, self.sems, self.view, self.other, self.own, self.axis, self.lanes = place, sems, view, other_view, own, axis, lanes

    def a1(self):
        p, q = self.place.at(self.axis, 0), self.place.at(1 - self.axis, 0)
        mine = self.view(*order(self.axis, p, q), None)
        self.sent_a = [self.sems.copy(self.own, mine, self.place.hop(self.axis, d)) for d in (1, -1)]

    def a2(self):
        q = self.place.at(1 - self.axis, 0)
        self.fwd_a = []
        for copy, d, part in zip(self.sent_a, (1, -1), halves(self.lanes), strict=True):
            copy.wait_recv()
            got = self.view(*order(self.axis, self.place.at(self.axis, -d), q), part)
            self.fwd_a.append(self.sems.copy(got, got, self.place.hop(self.axis, d)))

    def slab(self, q, half=None):
        n = self.place.side
        run = pl.ds(0, n) if half is None else pl.ds(half * (n // 2), n // 2)
        return self.view(*order(self.axis, run, q), None)

    def b1(self):
        for copy in self.fwd_a:
            copy.wait_recv()
        mine = self.slab(self.place.at(1 - self.axis, 0))
        self.sent_b = [self.sems.copy(mine, mine, self.place.hop(1 - self.axis, d)) for d in (1, -1)]
        self.to_partner = [self.sems.copy(mine, mine, self.place.partner)]

    def b2(self):
        self.fwd_b = []
        for copy, d, half in zip(self.sent_b, (1, -1), (0, 1), strict=True):
            copy.wait_recv()
            q = self.place.at(1 - self.axis, -d)
            got = self.slab(q, half)
            self.fwd_b.append(self.sems.copy(got, got, self.place.hop(1 - self.axis, d)))
            whole = self.slab(q)
            self.to_partner.append(self.sems.copy(whole, whole, self.place.partner))

    def c1(self):
        for copy, d, half in zip(self.fwd_b, (1, -1), (0, 1), strict=True):
            copy.wait_recv()
            got = self.slab(self.place.at(1 - self.axis, -2 * d), half)
            self.to_partner.append(self.sems.copy(got, got, self.place.partner))

    def end(self):
        for copy in self.to_partner:
            copy.wait_recv()


COPIES = 13


def gather_phases(place, send, recv, local, shards, outs, praw, blk, layers):
    wg, wu, wd = shards
    c = place.c
    sems = Sems(send, recv)
    half = wg.shape[-1] // 2
    rows = wg.shape[1]
    flows, raws, copies = [], [], []

    def p0():
        for j, w in enumerate((wg, wu)):
            raws.append(sems.copy(w, praw.at[j], place.partner))

    def down_rows():
        n = wd.shape[1]
        first = (n // 8 + 1) // 2 * 8
        return ((0, first), (first, n - first))

    def p1():
        x, y = place.xy
        for k, l in enumerate(layers):
            for j, (lo, n) in enumerate(down_rows()):
                def view(xs, ys, part, k=k, lo=lo, n=n):
                    lanes = ALL if part is None else pl.ds(*part)
                    return outs[2].at[k, xs, ys, c, pl.ds(lo, n), lanes]
                own = wd.at[l, pl.ds(lo, n)]
                copies.append(pltpu.make_async_copy(own, view(x, y, None), local.at[len(copies)]))
                copies[-1].start()
                flows.append(Gather(place, sems, view, None, own, j, wd.shape[-1]))
                flows[-1].a1()
        for j, w in enumerate((wg, wu)):
            raws[j].wait_recv()
            for k, l in enumerate(layers):
                for cc in (0, 1):
                    @pl.when(c == cc)
                    def _(cc=cc, j=j, w=w, k=k, l=l):
                        cols = slice(cc * half, (cc + 1) * half)
                        both = (w[l, :, cols].astype(F32), praw[j, l, :, cols].astype(F32))
                        blk[j, k] = jnp.concatenate(both if cc == 0 else both[::-1], axis=0).astype(BF16)
        for k, l in enumerate(layers):
            for j in (0, 1):
                def view(xs, ys, part, k=k, j=j):
                    lo, n = (0, half) if part is None else part
                    lanes = pl.ds(pl.multiple_of(c * half + lo, 128), n)
                    return outs[j].at[k, xs, ys, :, lanes]
                own = blk.at[j, k]
                copies.append(pltpu.make_async_copy(own, view(x, y, None), local.at[len(copies)]))
                copies[-1].start()
                flows.append(Gather(place, sems, view, None, own, j, half))
                flows[-1].a1()

    def every(step):
        def run():
            for flow in flows:
                getattr(flow, step)()
        return run

    def b1():
        for copy in copies:
            copy.wait()
        every("b1")()

    def end():
        every("end")()
        sems.finish()

    return [p0, p1, every("a2"), b1, every("b2"), every("c1"), end]


def gather(n, layers, wg, wu, wd, cid):
    side = math.isqrt(n // 2)
    L, rows, F = wg.shape
    drows, D = wd.shape[1:]
    k = len(layers)
    count = 2 + 4 * k * COPIES

    def kernel(wg, wu, wd, og, ou, od, praw, blk, send, recv, local):
        place = Place(n)
        place.greet()
        for phase in gather_phases(place, send, recv, local, (wg, wu, wd), (og, ou, od), praw, blk, layers):
            phase()

    out = pl.pallas_call(
        kernel,
        out_shape=[jax.ShapeDtypeStruct((k, side, side, 2 * rows, F), BF16)] * 2
        + [jax.ShapeDtypeStruct((k, side, side, 2, drows, D), BF16)],
        in_specs=[pl.BlockSpec(memory_space=pltpu.VMEM)] * 2 + [pl.BlockSpec(memory_space=pltpu.HBM)],
        out_specs=[pl.BlockSpec(memory_space=pltpu.HBM)] * 3,
        scratch_shapes=[
            pltpu.VMEM((2, L, rows, F), BF16),
            pltpu.VMEM((2, k, 2 * rows, F // 2), BF16),
            pltpu.SemaphoreType.DMA((count,)),
            pltpu.SemaphoreType.DMA((count,)),
            pltpu.SemaphoreType.DMA((4 * k,)),
        ],
        compiler_params=pltpu.CompilerParams(collective_id=cid, has_side_effects=True, vmem_limit_bytes=60 << 20),
        name=f"gather{cid}",
    )(wg, wu, wd)
    return [t.reshape(k, n * rows, F) for t in out[:2]] + [out[2].reshape(k, n * drows, D)]


class Scatter:
    def __init__(self, place, sems, axis, own, l1, part_a, full_a, total, snd_b, part_b, full_b):
        self.place, self.sems, self.axis = place, sems, axis
        self.own, self.l1, self.part_a, self.full_a, self.total, self.snd_b, self.part_b, self.full_b = (
            own, l1, part_a, full_a, total, snd_b, part_b, full_b)
        self.w = own.shape[-1]

    def idx(self, a, b):
        return order(self.axis, a, b)

    def pair(self, a, b):
        i = self.idx(a, b)
        return self.own[i].astype(F32) + self.l1[i].astype(F32)

    def loop(self, lo, n, body):
        lax.fori_loop(lo, lo + n, lambda j, _: (body(j), 0)[1], 0)

    def a1(self):
        n = self.place.side
        far = self.place.at(self.axis, 2)

        def body(j):
            self.own[self.idx(far, j)] = self.pair(far, j).astype(BF16)

        self.loop(0, n, body)
        self.sent_a = [
            self.sems.copy(self.own.at[self.idx(far, pl.ds(h * (n // 2), n // 2))], self.part_a.at[h], self.place.hop(self.axis, d))
            for h, d in enumerate((1, -1))
        ]

    def a2(self):
        n = self.place.side
        self.fwd_a = []
        for h, d in enumerate((1, -1)):
            to = self.place.at(self.axis, d)
            lo, rest = h * (n // 2), (1 - h) * (n // 2)

            def plain(j, to=to):
                self.own[self.idx(to, j)] = self.pair(to, j).astype(BF16)

            self.loop(rest, n // 2, plain)
            self.sent_a[h].wait_recv()

            def added(j, to=to, h=h, lo=lo):
                self.own[self.idx(to, j)] = (self.pair(to, j) + self.part_a[h, j - lo].astype(F32)).astype(BF16)

            self.loop(lo, n // 2, added)
            self.fwd_a.append(self.sems.copy(self.own.at[self.idx(to, pl.ds(0, n))], self.full_a.at[h], self.place.hop(self.axis, d)))

    def b1(self):
        n = self.place.side
        p = self.place.at(self.axis, 0)
        for copy in self.fwd_a:
            copy.wait_recv()

        def body(j):
            self.total[j] = self.pair(p, j) + self.full_a[0, j].astype(F32) + self.full_a[1, j].astype(F32)

        self.loop(0, n, body)
        far = self.place.at(1 - self.axis, 2)
        self.snd_b[far] = self.total[far].astype(BF16)
        self.sent_b = [
            self.sems.copy(self.snd_b.at[far, :, pl.ds(*part)], self.part_b.at[h, :, pl.ds(*part)], self.place.hop(1 - self.axis, d))
            for h, (d, part) in enumerate(zip((1, -1), halves(self.w), strict=True))
        ]

    def b2(self):
        self.fwd_b = []
        for h, (d, part) in enumerate(zip((1, -1), halves(self.w), strict=True)):
            to = self.place.at(1 - self.axis, d)
            lo, w = part
            rest = slice(w, self.w) if lo == 0 else slice(0, lo)
            got = slice(lo, lo + w)
            self.snd_b[to, :, rest] = self.total[to, :, rest].astype(BF16)
            self.sent_b[h].wait_recv()
            self.snd_b[to, :, got] = (self.total[to, :, got] + self.part_b[h, :, got].astype(F32)).astype(BF16)
            self.fwd_b.append(self.sems.copy(self.snd_b.at[to], self.full_b.at[h], self.place.hop(1 - self.axis, d)))

    def last(self):
        for copy in self.fwd_b:
            copy.wait_recv()
        return self.total[self.place.at(1 - self.axis, 0)] + self.full_b[0].astype(F32) + self.full_b[1].astype(F32)


def scatter_scratch(side, r, w):
    return [
        pltpu.VMEM((side, side, r, w), BF16),
        pltpu.VMEM((side, side, r, w), BF16),
        pltpu.VMEM((2, side // 2, r, w), BF16),
        pltpu.VMEM((2, side, r, w), BF16),
        pltpu.VMEM((side, r, w), F32),
        pltpu.VMEM((side, r, w), BF16),
        pltpu.VMEM((2, r, w), BF16),
        pltpu.VMEM((2, r, w), BF16),
    ]


def down_split(drows):
    first = (drows // 8 + 1) // 2 * 8
    return ((0, first), (first, drows - first))


def scatter_phases(place, send, recv, local, terms, outs, swap, bufs):
    c = place.c
    sems = Sems(send, recv)
    half = terms[0].shape[-1] // 2
    drows = terms[2].shape[3]
    (lo0, n0), (lo1, n1) = down_split(drows)

    def cols(j, who):
        return terms[j].at[:, :, :, pl.ds(pl.multiple_of(who * half, 128), half)]

    def share(who):
        return [
            terms[2].at[:, :, who, pl.ds(lo0, n0), :],
            terms[2].at[:, :, who, pl.ds(lo1, n1), :],
            cols(0, who),
            cols(1, who),
        ]

    axes = (0, 1, 0, 1)
    flows = [Scatter(place, sems, axis, *buf) for axis, buf in zip(axes, bufs, strict=True)]
    first, loads = [], []

    def p0():
        for k, (mine, theirs, flow) in enumerate(zip(share(c), share(1 - c), flows, strict=True)):
            first.append(sems.copy(theirs, flow.l1, place.partner))
            loads.append(pltpu.make_async_copy(mine, flow.own, local.at[k]))
            loads[-1].start()

    def a1():
        for flow, got, load in zip(flows, first, loads, strict=True):
            load.wait()
            got.wait_recv()
            flow.a1()

    def every(step):
        def run():
            for flow in flows:
                getattr(flow, step)()
        return run

    def end():
        rows = outs[0].shape[0]
        outs[2][pl.ds(lo0, n0), :] = flows[0].last().astype(BF16)
        outs[2][pl.ds(lo1, n1), :] = flows[1].last().astype(BF16)
        swaps = []
        for j in (0, 1):
            block = flows[2 + j].last()
            parts = (block[:rows].astype(BF16), block[rows:].astype(BF16))
            for cc in (0, 1):
                @pl.when(c == cc)
                def _(cc=cc, parts=parts, j=j):
                    outs[j][:, cc * half : (cc + 1) * half] = parts[cc]
                    swap[j] = parts[1 - cc]
            lanes = pl.ds(pl.multiple_of(c * half, 128), half)
            swaps.append(sems.copy(swap.at[j], outs[j].at[:, lanes], place.partner))
        for copy in swaps:
            copy.wait_recv()
        sems.finish()

    return [p0, a1, every("a2"), every("b1"), every("b2"), end]


def scatter(n, dwg, dwu, dwd, cid):
    side = math.isqrt(n // 2)
    D, F = dwg.shape
    rows, drows = D // n, F // n
    (_, n0), (_, n1) = down_split(drows)
    shapes = [(n0, D), (n1, D), (2 * rows, F // 2), (2 * rows, F // 2)]
    scratch = [scatter_scratch(side, r, w) for r, w in shapes]
    each = len(scratch[0])
    count = 4 * 9 + 2

    def kernel(dwg, dwu, dwd, og, ou, od, swap, send, recv, local, *flat):
        place = Place(n)
        place.greet()
        bufs = [flat[i * each : (i + 1) * each] for i in range(4)]
        for phase in scatter_phases(place, send, recv, local, (dwg, dwu, dwd), (og, ou, od), swap, bufs):
            phase()

    return pl.pallas_call(
        kernel,
        out_shape=[jax.ShapeDtypeStruct((rows, F), BF16)] * 2 + [jax.ShapeDtypeStruct((drows, D), BF16)],
        in_specs=[pl.BlockSpec(memory_space=pltpu.HBM)] * 3,
        out_specs=[pl.BlockSpec(memory_space=pltpu.VMEM)] * 3,
        scratch_shapes=[
            pltpu.VMEM((2, rows, F // 2), BF16),
            pltpu.SemaphoreType.DMA((count,)),
            pltpu.SemaphoreType.DMA((count,)),
            pltpu.SemaphoreType.DMA((4,)),
        ]
        + [s for group in scratch for s in group],
        compiler_params=pltpu.CompilerParams(collective_id=cid, has_side_effects=True, vmem_limit_bytes=60 << 20),
        name=f"scatter{cid}",
    )(dwg.reshape(side, side, 2 * rows, F), dwu.reshape(side, side, 2 * rows, F), dwd.reshape(side, side, 2, drows, D))


def dot(a, b, dims=((1,), (0,))):
    return lax.dot_general(a, b, (dims, ((), ())), preferred_element_type=F32)


def normed(h):
    wide = h.astype(F32)
    scale = lax.rsqrt(jnp.mean(wide**2, -1, keepdims=True) + 1e-6)
    return (wide * scale).astype(BF16)


def layer(h, wg, wu, wd):
    a = normed(h)
    gate, up = dot(a, wg), dot(a, wu)
    return h + dot((jax.nn.silu(gate) * up).astype(BF16), wd).astype(BF16)


def solution(mesh):
    n = mesh.shape["dp"]

    def device(x, dy, wg, wu, wd):
        layers = range(wg.shape[0])
        gg, gu, gd = gather(n, tuple(layers), wg, wu, wd, 0)

        def stack(weights, h):
            for w in weights:
                h = layer(h, *w)
            return h

        weights = [(gg[l], gu[l], gd[l]) for l in layers]
        _, back = jax.vjp(stack, weights, x[0])
        by_weights, by_x = back(dy[0])
        parts = [scatter(n, *by_weights[l], 1) for l in reversed(layers)][::-1]
        return (by_x[None], *(jnp.stack([p[j] for p in parts]) for j in range(3)))

    tokens, rows = P(("rep", "dp")), P(None, "dp")
    return jax.shard_map(
        device, mesh=mesh, in_specs=(tokens, tokens, rows, rows, rows), out_specs=(tokens, *[P("rep", "dp")] * 3), check_vma=False
    )
```

```python
import functools
import math
import jax
import jax.numpy as jnp
from jax import lax
from jax.experimental import pallas as pl
from jax.experimental.pallas import tpu as pltpu
from jax.sharding import PartitionSpec as P

MESH = pl.DeviceIdType.MESH
F32, BF16 = jnp.float32, jnp.bfloat16
ALL = slice(None)


def halves(n):
    first = (n // 128 + 1) // 2 * 128
    return (0, first), (first, n - first)


class Place:
    def __init__(self, n):
        self.side = math.isqrt(n // 2)
        me = lax.axis_index("dp")
        chip = me // 2
        self.c = me % 2
        self.xy = (chip // self.side, chip % self.side)
        self.partner = {"dp": chip * 2 + 1 - self.c}
        self.places = {(a, d): lax.rem(self.xy[a] + d + self.side, self.side) for a in (0, 1) for d in range(-2, 3)}
        self.hops = {}
        for a in (0, 1):
            for d in (1, -1):
                xy = list(self.xy)
                xy[a] = self.places[a, d]
                self.hops[a, d] = {"dp": (xy[0] * self.side + xy[1]) * 2 + self.c}

    def hop(self, axis, by):
        return self.hops[axis, by]

    def at(self, axis, by):
        return self.places[axis, by]

    def greet(self):
        barrier = pltpu.get_barrier_semaphore()
        others = [self.partner] + [self.hop(a, d) for a in (0, 1) for d in (1, -1)]
        for other in others:
            pl.semaphore_signal(barrier, inc=1, device_id=other, device_id_type=MESH)
        pl.semaphore_wait(barrier, len(others))


class Sems:
    def __init__(self, send, recv):
        self.send, self.recv, self.used, self.started = send, recv, 0, []

    def copy(self, src, dst, to):
        k = self.used
        self.used += 1
        made = pltpu.make_async_remote_copy(
            src_ref=src, dst_ref=dst, send_sem=self.send.at[k], recv_sem=self.recv.at[k], device_id=to, device_id_type=MESH
        )
        self.started.append(made)
        return made

    def finish(self):
        for made in self.started:
            made.wait_send()


def order(axis, a, b):
    return (a, b) if axis == 0 else (b, a)


class Gather:
    def __init__(self, place, sems, view, own, axis, lanes):
        n, other = place.side, 1 - axis
        p, q = place.at(axis, 0), place.at(other, 0)

        def slab(q, half=None):
            run = pl.ds(0, n) if half is None else pl.ds(half * (n // 2), n // 2)
            return view(*order(axis, run, q), None)

        self.sent_a, self.fwd_a, self.sent_b, self.fwd_b, self.swap = [], [], [], [], []
        mine = slab(q)
        self.swap.append(sems.copy(mine, mine, place.partner))
        for half, (d, part) in enumerate(zip((1, -1), halves(lanes), strict=True)):
            self.sent_a.append(sems.copy(own, view(*order(axis, p, q), None), place.hop(axis, d)))
            got = view(*order(axis, place.at(axis, -d), q), part)
            self.fwd_a.append(sems.copy(got, got, place.hop(axis, d)))
            self.sent_b.append(sems.copy(mine, mine, place.hop(other, d)))
            got = slab(place.at(other, -d), half)
            self.fwd_b.append(sems.copy(got, got, place.hop(other, d)))
            whole = slab(place.at(other, -d))
            self.swap.append(sems.copy(whole, whole, place.partner))
            got = slab(place.at(other, -2 * d), half)
            self.swap.append(sems.copy(got, got, place.partner))

    def a1(self):
        for copy in self.sent_a:
            copy.start()

    def a2(self):
        for k in (0, 1):
            self.sent_a[k].wait_recv()
            self.fwd_a[k].start()

    def b1(self):
        for copy in self.fwd_a:
            copy.wait_recv()
        for copy in self.sent_b:
            copy.start()
        self.swap[0].start()

    def b2(self):
        for k in (0, 1):
            self.sent_b[k].wait_recv()
            self.fwd_b[k].start()
            self.swap[1 + 2 * k].start()

    def c1(self):
        for k in (0, 1):
            self.fwd_b[k].wait_recv()
            self.swap[2 + 2 * k].start()

    def end(self):
        for copy in self.swap:
            copy.wait_recv()


def down_split(drows):
    first = (drows // 8 + 1) // 2 * 8
    return ((0, first), (first, drows - first))


COPIES = 13


def gather_phases(place, send, recv, local, shards, outs, praw, blk, layers):
    wg, wu, wd = shards
    c = place.c
    sems = Sems(send, recv)
    half = wg.shape[-1] // 2
    rows = wg.shape[1]
    flows, copies = [], []
    x, y = place.xy
    raws = [sems.copy(w, praw.at[1, j], place.partner) for j, w in enumerate((wg, wu))]
    loads = [pltpu.make_async_copy(w, praw.at[0, j], local.at[4 * len(layers) + j]) for j, w in enumerate((wg, wu))]
    at_once = 2 * len(layers)

    def add(own, view, axis, lanes):
        copies.append(pltpu.make_async_copy(own, view(x, y, None), local.at[len(copies)]))
        flows.append(Gather(place, sems, view, own, axis, lanes))

    for k, l in enumerate(layers):
        for j, (lo, m) in enumerate(down_split(wd.shape[1])):
            def view(xs, ys, part, k=k, lo=lo, m=m):
                lanes = ALL if part is None else pl.ds(*part)
                return outs[2].at[k, xs, ys, c, pl.ds(lo, m), lanes]
            add(wd.at[l, pl.ds(lo, m)], view, j, wd.shape[-1])
    for k in range(len(layers)):
        for j in (0, 1):
            def view(xs, ys, part, k=k, j=j):
                lo, m = (0, half) if part is None else part
                return outs[j].at[k, xs, ys, :, pl.ds(pl.multiple_of(c * half + lo, 128), m)]
            add(blk.at[j, k], view, j, half)

    def p0():
        for copy in raws + loads:
            copy.start()
        for copy, flow in zip(copies[:at_once], flows[:at_once], strict=True):
            copy.start()
            flow.a1()

    def p1():
        for j in (0, 1):
            loads[j].wait()
            raws[j].wait_recv()
            for k, l in enumerate(layers):
                for cc in (0, 1):
                    @pl.when(c == cc)
                    def _(cc=cc, j=j, k=k, l=l):
                        cols = slice(cc * half, (cc + 1) * half)
                        both = (praw[0, j, l, :, cols].astype(F32), praw[1, j, l, :, cols].astype(F32))
                        blk[j, k] = jnp.concatenate(both if cc == 0 else both[::-1], axis=0).astype(BF16)
        for copy, flow in zip(copies[at_once:], flows[at_once:], strict=True):
            copy.start()
            flow.a1()

    def every(step):
        def run():
            for flow in flows:
                getattr(flow, step)()
        return run

    def b1():
        for copy in copies:
            copy.wait()
        every("b1")()

    def end():
        every("end")()
        sems.finish()

    return [p0, p1, every("a2"), b1, every("b2"), every("c1"), end]


def gather(n, layers, wg, wu, wd, cid):
    side = math.isqrt(n // 2)
    L, rows, F = wg.shape
    drows, D = wd.shape[1:]
    k = len(layers)
    count = 2 + 4 * k * COPIES

    def kernel(wg, wu, wd, og, ou, od, praw, blk, send, recv, local):
        place = Place(n)
        place.greet()
        for phase in gather_phases(place, send, recv, local, (wg, wu, wd), (og, ou, od), praw, blk, layers):
            phase()

    out = pl.pallas_call(
        kernel,
        out_shape=[jax.ShapeDtypeStruct((k, side, side, 2 * rows, F), BF16)] * 2
        + [jax.ShapeDtypeStruct((k, side, side, 2, drows, D), BF16)],
        in_specs=[pl.BlockSpec(memory_space=pltpu.HBM)] * 3,
        out_specs=[pl.BlockSpec(memory_space=pltpu.HBM)] * 3,
        scratch_shapes=[
            pltpu.VMEM((2, 2, L, rows, F), BF16),
            pltpu.VMEM((2, k, 2 * rows, F // 2), BF16),
            pltpu.SemaphoreType.DMA((count,)),
            pltpu.SemaphoreType.DMA((count,)),
            pltpu.SemaphoreType.DMA((4 * k + 2,)),
        ],
        compiler_params=pltpu.CompilerParams(collective_id=cid, has_side_effects=True, vmem_limit_bytes=60 << 20),
        name=f"gather{cid}",
    )(wg, wu, wd)
    return [t.reshape(k, n * rows, F) for t in out[:2]] + [out[2].reshape(k, n * drows, D)]


class Scatter:
    def __init__(self, place, sems, axis, own, l1, part_a, full_a, total, snd_b, part_b, full_b):
        self.place, self.sems, self.axis = place, sems, axis
        self.own, self.l1, self.part_a, self.full_a, self.total, self.snd_b, self.part_b, self.full_b = (
            own, l1, part_a, full_a, total, snd_b, part_b, full_b)
        self.w = own.shape[-1]
        n, other = place.side, 1 - axis
        far_a, far_b = place.at(axis, 2), place.at(other, 2)
        self.sent_a, self.fwd_a, self.sent_b, self.fwd_b = [], [], [], []
        for h, (d, part) in enumerate(zip((1, -1), halves(self.w), strict=True)):
            run = pl.ds(h * (n // 2), n // 2)
            self.sent_a.append(sems.copy(own.at[order(axis, far_a, run)], part_a.at[h], place.hop(axis, d)))
            to = place.at(axis, d)
            self.fwd_a.append(sems.copy(own.at[order(axis, to, pl.ds(0, n))], full_a.at[h], place.hop(axis, d)))
            lanes = pl.ds(*part)
            self.sent_b.append(sems.copy(snd_b.at[far_b, :, lanes], part_b.at[h, :, lanes], place.hop(other, d)))
            self.fwd_b.append(sems.copy(snd_b.at[place.at(other, d)], full_b.at[h], place.hop(other, d)))

    def idx(self, a, b):
        return order(self.axis, a, b)

    def pair(self, a, b):
        i = self.idx(a, b)
        return self.own[i].astype(F32) + self.l1[i].astype(F32)

    def loop(self, lo, n, body):
        lax.fori_loop(lo, lo + n, lambda j, _: (body(j), 0)[1], 0)

    def a1(self):
        n = self.place.side
        far = self.place.at(self.axis, 2)

        def body(j):
            self.own[self.idx(far, j)] = self.pair(far, j).astype(BF16)

        self.loop(0, n, body)
        for copy in self.sent_a:
            copy.start()

    def a2(self):
        n = self.place.side
        for h, d in enumerate((1, -1)):
            to = self.place.at(self.axis, d)
            lo, rest = h * (n // 2), (1 - h) * (n // 2)

            def plain(j, to=to):
                self.own[self.idx(to, j)] = self.pair(to, j).astype(BF16)

            self.loop(rest, n // 2, plain)
            self.sent_a[h].wait_recv()

            def added(j, to=to, h=h, lo=lo):
                self.own[self.idx(to, j)] = (self.pair(to, j) + self.part_a[h, j - lo].astype(F32)).astype(BF16)

            self.loop(lo, n // 2, added)
            self.fwd_a[h].start()

    def b1(self):
        n = self.place.side
        p = self.place.at(self.axis, 0)
        for copy in self.fwd_a:
            copy.wait_recv()

        def body(j):
            self.total[j] = self.pair(p, j) + self.full_a[0, j].astype(F32) + self.full_a[1, j].astype(F32)

        self.loop(0, n, body)
        far = self.place.at(1 - self.axis, 2)
        self.snd_b[far] = self.total[far].astype(BF16)
        for copy in self.sent_b:
            copy.start()

    def b2(self):
        for h, (d, part) in enumerate(zip((1, -1), halves(self.w), strict=True)):
            to = self.place.at(1 - self.axis, d)
            lo, w = part
            rest = slice(w, self.w) if lo == 0 else slice(0, lo)
            got = slice(lo, lo + w)
            self.snd_b[to, :, rest] = self.total[to, :, rest].astype(BF16)
            self.sent_b[h].wait_recv()
            self.snd_b[to, :, got] = (self.total[to, :, got] + self.part_b[h, :, got].astype(F32)).astype(BF16)
            self.fwd_b[h].start()

    def last(self):
        for copy in self.fwd_b:
            copy.wait_recv()
        return self.total[self.place.at(1 - self.axis, 0)] + self.full_b[0].astype(F32) + self.full_b[1].astype(F32)


def scatter_scratch(side, r, w):
    return [
        pltpu.VMEM((side, side, r, w), BF16),
        pltpu.VMEM((side, side, r, w), BF16),
        pltpu.VMEM((2, side // 2, r, w), BF16),
        pltpu.VMEM((2, side, r, w), BF16),
        pltpu.VMEM((side, r, w), F32),
        pltpu.VMEM((side, r, w), BF16),
        pltpu.VMEM((2, r, w), BF16),
        pltpu.VMEM((2, r, w), BF16),
    ]


def scatter_phases(place, send, recv, local, terms, outs, swap, bufs):
    c = place.c
    sems = Sems(send, recv)
    half = terms[0].shape[-1] // 2
    drows = terms[2].shape[3]
    (lo0, n0), (lo1, n1) = down_split(drows)

    def cols(j, who):
        return terms[j].at[:, :, :, pl.ds(pl.multiple_of(who * half, 128), half)]

    def share(who):
        return [
            terms[2].at[:, :, who, pl.ds(lo0, n0), :],
            terms[2].at[:, :, who, pl.ds(lo1, n1), :],
            cols(0, who),
            cols(1, who),
        ]

    axes = (0, 1, 0, 1)
    flows = [Scatter(place, sems, axis, *buf) for axis, buf in zip(axes, bufs, strict=True)]
    first = [sems.copy(theirs, flow.l1, place.partner) for theirs, flow in zip(share(1 - c), flows, strict=True)]
    loads = [pltpu.make_async_copy(mine, flow.own, local.at[k]) for k, (mine, flow) in enumerate(zip(share(c), flows, strict=True))]
    swaps = [sems.copy(swap.at[0, j], swap.at[1, j], place.partner) for j in (0, 1)]

    def p0():
        for copy in first + loads:
            copy.start()

    def a1():
        for flow, got, load in zip(flows, first, loads, strict=True):
            load.wait()
            got.wait_recv()
            flow.a1()

    def every(step):
        def run():
            for flow in flows:
                getattr(flow, step)()
        return run

    def end():
        rows = outs[0].shape[0]
        outs[2][pl.ds(lo0, n0), :] = flows[0].last().astype(BF16)
        outs[2][pl.ds(lo1, n1), :] = flows[1].last().astype(BF16)
        for j in (0, 1):
            block = flows[2 + j].last()
            parts = (block[:rows].astype(BF16), block[rows:].astype(BF16))
            for cc in (0, 1):
                @pl.when(c == cc)
                def _(cc=cc, parts=parts, j=j):
                    outs[j][:, cc * half : (cc + 1) * half] = parts[cc]
                    swap[0, j] = parts[1 - cc]
            swaps[j].start()
        for j, copy in enumerate(swaps):
            copy.wait_recv()
            for cc in (0, 1):
                @pl.when(c == cc)
                def _(cc=cc, j=j):
                    outs[j][:, (1 - cc) * half : (2 - cc) * half] = swap[1, j]
        sems.finish()

    return [p0, a1, every("a2"), every("b1"), every("b2"), end]


def scatter_parts(n, dwg, dwu, dwd):
    side = math.isqrt(n // 2)
    D, F = dwg.shape
    rows, drows = D // n, F // n
    (_, n0), (_, n1) = down_split(drows)
    shapes = [(n0, D), (n1, D), (2 * rows, F // 2), (2 * rows, F // 2)]
    groups = [scatter_scratch(side, r, w) for r, w in shapes]
    count = 4 * 9 + 2
    operands = [dwg.reshape(side, side, 2 * rows, F), dwu.reshape(side, side, 2 * rows, F), dwd.reshape(side, side, 2, drows, D)]
    outs = [jax.ShapeDtypeStruct((rows, F), BF16)] * 2 + [jax.ShapeDtypeStruct((drows, D), BF16)]
    scratch = [
        pltpu.VMEM((2, 2, rows, F // 2), BF16),
        pltpu.SemaphoreType.DMA((count,)),
        pltpu.SemaphoreType.DMA((count,)),
        pltpu.SemaphoreType.DMA((4,)),
    ] + [s for group in groups for s in group]
    return operands, outs, [pl.BlockSpec(memory_space=pltpu.VMEM)] * 3, scratch, len(groups[0])


def scatter(n, dwg, dwu, dwd, cid):
    operands, outs, out_specs, scratch, each = scatter_parts(n, dwg, dwu, dwd)

    def kernel(dwg, dwu, dwd, og, ou, od, swap, send, recv, local, *flat):
        place = Place(n)
        place.greet()
        bufs = [flat[i * each : (i + 1) * each] for i in range(4)]
        for phase in scatter_phases(place, send, recv, local, (dwg, dwu, dwd), (og, ou, od), swap, bufs):
            phase()

    return pl.pallas_call(
        kernel,
        out_shape=outs,
        in_specs=[pl.BlockSpec(memory_space=pltpu.HBM)] * 3,
        out_specs=out_specs,
        scratch_shapes=scratch,
        compiler_params=pltpu.CompilerParams(collective_id=cid, has_side_effects=True, vmem_limit_bytes=60 << 20),
        name=f"scatter{cid}",
    )(*operands)


def dot(a, b, dims=((1,), (0,))):
    return lax.dot_general(a, b, (dims, ((), ())), preferred_element_type=F32)


ROWS_ROWS, COLS_COLS = ((0,), (0,)), ((1,), (1,))


def sigmoid(t):
    return 0.5 * jnp.tanh(0.5 * t) + 0.5


def scale_of(wide):
    return lax.rsqrt(jnp.mean(wide * wide, -1, keepdims=True) + 1e-6)


def normed(h):
    wide = h.astype(F32)
    return (wide * scale_of(wide)).astype(BF16)


def cut(n, most):
    return max(c for c in range(256, most + 1, 256) if n % c == 0)


def at_steps(phases, steps, step):
    for phase, k in zip(phases, steps, strict=True):
        pl.when(step == k)(phase)


HBM = pl.BlockSpec(memory_space=pltpu.HBM)
LIMIT = 62 << 20


def once(shape, index):
    return pl.BlockSpec(shape, index, pipeline_mode=pl.Buffered(1))


def forward(n, h, wg, wu, wd, shards, layer, cid):
    S, D = h.shape
    F = wg.shape[1]
    T, C = cut(S, 512), cut(F, 768)
    nt, nc = S // T, F // C
    side = math.isqrt(n // 2)
    L, rows, _ = shards[0].shape
    drows = shards[2].shape[1]
    count = 2 + 4 * COPIES
    steps = nt * nc
    when = [0, 1, 3, 5, steps - 2, steps, steps]

    def kernel(h, wg, wu, wd, sg, su, sd, o, og, ou, od, a, acc, praw, blk, send, recv, local):
        j = pl.program_id(1)
        step = pl.program_id(0) * nc + j
        place = Place(n)
        pl.when(step == 0)(place.greet)
        phases = gather_phases(place, send, recv, local, (sg, su, sd), (og, ou, od), praw, blk, (layer,))
        for phase, k in zip(phases, when, strict=True):
            if k < steps:
                pl.when(step == k)(phase)

        @pl.when(j == 0)
        def _():
            a[...] = normed(h[...])
            acc[...] = jnp.zeros_like(acc)

        gate, up = dot(a[...], wg[...]), dot(a[...], wu[...])
        act = (gate * sigmoid(gate) * up).astype(BF16)
        acc[...] += dot(act, wd[...])

        @pl.when(j == nc - 1)
        def _():
            o[...] = (h[...].astype(F32) + acc[...].astype(BF16).astype(F32)).astype(BF16)

        @pl.when(step == steps - 1)
        def _():
            for phase, k in zip(phases, when, strict=True):
                if k >= steps:
                    phase()

    flops = 6 * S * D * F
    out = pl.pallas_call(
        kernel,
        grid=(nt, nc),
        out_shape=[jax.ShapeDtypeStruct((S, D), BF16)]
        + [jax.ShapeDtypeStruct((1, side, side, 2 * rows, F), BF16)] * 2
        + [jax.ShapeDtypeStruct((1, side, side, 2, drows, D), BF16)],
        in_specs=[
            pl.BlockSpec((T, D), lambda i, j: (i, 0)),
            pl.BlockSpec((D, C), lambda i, j: (0, j)),
            pl.BlockSpec((D, C), lambda i, j: (0, j)),
            pl.BlockSpec((C, D), lambda i, j: (j, 0)),
            HBM,
            HBM,
            HBM,
        ],
        out_specs=[pl.BlockSpec((T, D), lambda i, j: (i, 0)), HBM, HBM, HBM],
        scratch_shapes=[
            pltpu.VMEM((T, D), BF16),
            pltpu.VMEM((T, D), F32),
            pltpu.VMEM((2, 2, L, rows, F), BF16),
            pltpu.VMEM((2, 1, 2 * rows, F // 2), BF16),
            pltpu.SemaphoreType.DMA((count,)),
            pltpu.SemaphoreType.DMA((count,)),
            pltpu.SemaphoreType.DMA((6,)),
        ],
        compiler_params=pltpu.CompilerParams(
            collective_id=cid, has_side_effects=True, vmem_limit_bytes=LIMIT, dimension_semantics=("arbitrary", "arbitrary")
        ),
        cost_estimate=pl.CostEstimate(flops=flops, bytes_accessed=4 * S * D, transcendentals=S * F),
        name="forward",
    )(h, wg, wu, wd, *shards)
    return out[0], (out[1].reshape(n * rows, F), out[2].reshape(n * rows, F), out[3].reshape(n * drows, D))


def backward(n, h, dy, wg, wu, wd, terms, cid):
    S, D = h.shape
    F = wg.shape[1]
    T, C = cut(S, 512), cut(F, 768)
    nt, nc = S // T, F // C
    steps = nt * nc
    when = [0, 2, 5, 9, 10, steps]
    if terms is None:
        more_in, more_out, more_specs, scratch, kind = [], [], [], [], {}
    else:
        more_in, more_out, more_specs, scratch, each = scatter_parts(n, *terms)
        kind = {"collective_id": cid, "has_side_effects": True}

    def kernel(h, dy, wg, wu, wd, *rest):
        terms_, rest = rest[: len(more_in)], rest[len(more_in) :]
        (act, dg, du, a, dh), rest = rest[:5], rest[5:]
        outs, rest = rest[: len(more_out)], rest[len(more_out) :]
        acc, rest = rest[0], rest[1:]
        j = pl.program_id(1)
        step = pl.program_id(0) * nc + j
        if terms is not None:
            place = Place(n)
            pl.when(step == 0)(place.greet)
            swap, send, recv, local, *flat = rest
            bufs = [flat[i * each : (i + 1) * each] for i in range(4)]
            phases = scatter_phases(place, send, recv, local, terms_, outs, swap, bufs)
            for phase, k in zip(phases, when, strict=True):
                if k < steps:
                    pl.when(step == k)(phase)

        @pl.when(j == 0)
        def _():
            a[...] = normed(h[...])
            acc[...] = jnp.zeros_like(acc)

        gate, up = dot(a[...], wg[...]), dot(a[...], wu[...])
        dact = dot(dy[...], wd[...], COLS_COLS).astype(BF16).astype(F32)
        sig = sigmoid(gate)
        silu = gate * sig
        act[...] = (silu * up).astype(BF16)
        by_up = (dact * silu).astype(BF16)
        by_gate = (dact * up * (sig + silu * (1.0 - sig))).astype(BF16)
        du[...] = by_up
        dg[...] = by_gate
        acc[...] += dot(by_gate, wg[...], COLS_COLS) + dot(by_up, wu[...], COLS_COLS)

        @pl.when(j == nc - 1)
        def _():
            by_a = acc[...].astype(BF16).astype(F32)
            wide = h[...].astype(F32)
            scale = scale_of(wide)
            hat = wide * scale
            by_wide = scale * (by_a - hat * jnp.mean(by_a * hat, -1, keepdims=True))
            dh[...] = (dy[...].astype(F32) + by_wide.astype(BF16).astype(F32)).astype(BF16)

        if terms is not None:
            @pl.when(step == steps - 1)
            def _():
                for phase, k in zip(phases, when, strict=True):
                    if k >= steps:
                        phase()

    tile = pl.BlockSpec((T, D), lambda i, j: (i, 0))
    wide_tile = pl.BlockSpec((T, C), lambda i, j: (i, j))
    out = pl.pallas_call(
        kernel,
        grid=(nt, nc),
        out_shape=[jax.ShapeDtypeStruct((S, F), BF16)] * 3 + [jax.ShapeDtypeStruct((S, D), BF16)] * 2 + more_out,
        in_specs=[
            tile,
            tile,
            pl.BlockSpec((D, C), lambda i, j: (0, j)),
            pl.BlockSpec((D, C), lambda i, j: (0, j)),
            pl.BlockSpec((C, D), lambda i, j: (j, 0)),
        ]
        + [HBM] * len(more_in),
        out_specs=[wide_tile] * 3 + [tile] * 2 + more_specs,
        scratch_shapes=[pltpu.VMEM((T, D), F32)] + scratch,
        compiler_params=pltpu.CompilerParams(vmem_limit_bytes=LIMIT, dimension_semantics=("arbitrary", "arbitrary"), **kind),
        cost_estimate=pl.CostEstimate(flops=10 * S * D * F, bytes_accessed=6 * S * F, transcendentals=S * F),
        name=f"backward{cid}",
    )(h, dy, wg, wu, wd, *more_in)
    return out[:5], out[5:]


def weights_kernel(a, dy, act, dg, du):
    S, D = a.shape
    F = act.shape[1]
    C = cut(F, 768)
    nc = F // C

    def kernel(a, dy, act, dg, du, og, ou, od):
        step = pl.program_id(0)

        @pl.when(step < nc)
        def _():
            od[...] = dot(act[...], dy[...], ROWS_ROWS).astype(BF16)

        @pl.when((step >= nc) & (step < 2 * nc))
        def _():
            og[...] = dot(a[...], dg[...], ROWS_ROWS).astype(BF16)

        @pl.when(step >= 2 * nc)
        def _():
            ou[...] = dot(a[...], du[...], ROWS_ROWS).astype(BF16)

    def at(k):
        return lambda i: jnp.clip(i - k * nc, 0, nc - 1)

    def cols(k, rows):
        f = at(k)
        return pl.BlockSpec((rows, C), lambda i: (0, f(i)))

    down = at(0)
    return pl.pallas_call(
        kernel,
        grid=(3 * nc,),
        out_shape=[jax.ShapeDtypeStruct((D, F), BF16)] * 2 + [jax.ShapeDtypeStruct((F, D), BF16)],
        in_specs=[once((S, D), lambda i: (0, 0))] * 2 + [cols(0, S), cols(1, S), cols(2, S)],
        out_specs=[cols(1, D), cols(2, D), pl.BlockSpec((C, D), lambda i: (down(i), 0))],
        compiler_params=pltpu.CompilerParams(vmem_limit_bytes=LIMIT, dimension_semantics=("arbitrary",)),
        cost_estimate=pl.CostEstimate(flops=6 * S * D * F, bytes_accessed=6 * S * F, transcendentals=0),
        name="weights",
    )(a, dy, act, dg, du)


def solution(mesh):
    n = mesh.shape["dp"]

    def device(x, dy, wg, wu, wd):
        shards = (wg, wu, wd)
        layers = wg.shape[0]
        x, dy = x.reshape(x.shape[1:]), dy.reshape(dy.shape[1:])
        states, weights = [x], [tuple(t[0] for t in gather(n, (0,), *shards, 0))]
        for l in range(layers - 1):
            h, more = forward(n, states[l], *weights[l], shards, l + 1, 1 + l)
            states.append(h)
            weights.append(more)
        terms, sums = None, []
        for l in reversed(range(layers)):
            (act, dg, du, a, dh), done = backward(n, states[l], dy, *weights[l], terms, layers + 1 + l)
            if terms is not None:
                sums.append(done)
            terms = weights_kernel(a, dy, act, dg, du)
            dy = dh
        sums.append(scatter(n, *terms, 2 * layers + 1))
        return (dy[None], *(jnp.stack([s[j] for s in sums[::-1]]) for j in range(3)))

    tokens, rows = P(("rep", "dp")), P(None, "dp")
    return jax.shard_map(
        device, mesh=mesh, in_specs=(tokens, tokens, rows, rows, rows), out_specs=(tokens, *[P("rep", "dp")] * 3), check_vma=False
    )
```

```python
import functools
import math
import jax
import jax.numpy as jnp
from jax import lax
from jax.experimental import pallas as pl
from jax.experimental.pallas import tpu as pltpu
from jax.sharding import PartitionSpec as P

MESH = pl.DeviceIdType.MESH
F32, BF16 = jnp.float32, jnp.bfloat16
ALL = slice(None)


def halves(n):
    first = (n // 128 + 1) // 2 * 128
    return (0, first), (first, n - first)


class Place:
    def __init__(self, n):
        self.side = math.isqrt(n // 2)
        me = lax.axis_index("dp")
        chip = me // 2
        self.c = me % 2
        self.xy = (chip // self.side, chip % self.side)
        self.partner = {"dp": chip * 2 + 1 - self.c}
        self.places = {(a, d): lax.rem(self.xy[a] + d + self.side, self.side) for a in (0, 1) for d in range(-2, 3)}
        self.hops = {}
        for a in (0, 1):
            for d in (1, -1):
                xy = list(self.xy)
                xy[a] = self.places[a, d]
                self.hops[a, d] = {"dp": (xy[0] * self.side + xy[1]) * 2 + self.c}

    def hop(self, axis, by):
        return self.hops[axis, by]

    def at(self, axis, by):
        return self.places[axis, by]

    def greet(self):
        barrier = pltpu.get_barrier_semaphore()
        others = [self.partner] + [self.hop(a, d) for a in (0, 1) for d in (1, -1)]
        for other in others:
            pl.semaphore_signal(barrier, inc=1, device_id=other, device_id_type=MESH)
        pl.semaphore_wait(barrier, len(others))


class Sems:
    def __init__(self, send, recv):
        self.send, self.recv, self.used, self.started = send, recv, 0, []

    def copy(self, src, dst, to):
        k = self.used
        self.used += 1
        made = pltpu.make_async_remote_copy(
            src_ref=src, dst_ref=dst, send_sem=self.send.at[k], recv_sem=self.recv.at[k], device_id=to, device_id_type=MESH
        )
        self.started.append(made)
        return made

    def finish(self):
        for made in self.started:
            made.wait_send()


def order(axis, a, b):
    return (a, b) if axis == 0 else (b, a)


class Gather:
    def __init__(self, place, sems, view, own, axis, lanes):
        n, other = place.side, 1 - axis
        p, q = place.at(axis, 0), place.at(other, 0)

        def slab(q, half=None):
            run = pl.ds(0, n) if half is None else pl.ds(half * (n // 2), n // 2)
            return view(*order(axis, run, q), None)

        self.sent_a, self.fwd_a, self.sent_b, self.fwd_b, self.swap = [], [], [], [], []
        mine = slab(q)
        self.swap.append(sems.copy(mine, mine, place.partner))
        for half, (d, part) in enumerate(zip((1, -1), halves(lanes), strict=True)):
            self.sent_a.append(sems.copy(own, view(*order(axis, p, q), None), place.hop(axis, d)))
            got = view(*order(axis, place.at(axis, -d), q), part)
            self.fwd_a.append(sems.copy(got, got, place.hop(axis, d)))
            self.sent_b.append(sems.copy(mine, mine, place.hop(other, d)))
            got = slab(place.at(other, -d), half)
            self.fwd_b.append(sems.copy(got, got, place.hop(other, d)))
            whole = slab(place.at(other, -d))
            self.swap.append(sems.copy(whole, whole, place.partner))
            got = slab(place.at(other, -2 * d), half)
            self.swap.append(sems.copy(got, got, place.partner))

    def a1(self):
        for copy in self.sent_a:
            copy.start()

    def a2(self):
        for k in (0, 1):
            self.sent_a[k].wait_recv()
            self.fwd_a[k].start()

    def b1(self):
        for copy in self.fwd_a:
            copy.wait_recv()
        for copy in self.sent_b:
            copy.start()
        self.swap[0].start()

    def b2(self):
        for k in (0, 1):
            self.sent_b[k].wait_recv()
            self.fwd_b[k].start()
            self.swap[1 + 2 * k].start()

    def c1(self):
        for k in (0, 1):
            self.fwd_b[k].wait_recv()
            self.swap[2 + 2 * k].start()

    def end(self):
        for copy in self.swap:
            copy.wait_recv()

    def got_a(self):
        for copy in self.fwd_a:
            copy.wait_recv()

    def b1_next(self):
        for copy in self.sent_b:
            copy.start()
        self.swap[0].start()

    def sends(self, first):
        for copy in self.sent_a + self.fwd_a if first else self.sent_b + self.fwd_b + self.swap:
            copy.wait_send()


def down_split(drows):
    first = (drows // 8 + 1) // 2 * 8
    return ((0, first), (first, drows - first))


COPIES = 13


def gather_flows(place, sems, outs, owns):
    c = place.c
    half = outs[0].shape[-1] // 2
    D = outs[2].shape[-1]
    flows, views = [], []
    for j, (lo, m) in enumerate(down_split(outs[2].shape[3])):
        def view(xs, ys, part, lo=lo, m=m):
            return outs[2].at[xs, ys, c, pl.ds(lo, m), ALL if part is None else pl.ds(*part)]
        views.append((view, j, D))
    for j in (0, 1):
        def view(xs, ys, part, j=j):
            lo, m = (0, half) if part is None else part
            return outs[j].at[xs, ys, :, pl.ds(pl.multiple_of(c * half + lo, 128), m)]
        views.append((view, j, half))
    mine = [view(*place.xy, None) for view, _, _ in views]
    flows = [Gather(place, sems, view, own, axis, lanes) for (view, axis, lanes), own in zip(views, owns or mine, strict=True)]
    return flows, mine


def gather_shapes(n, rows, F, drows, D):
    side = math.isqrt(n // 2)
    return [jax.ShapeDtypeStruct((side, side, 2 * rows, F), BF16)] * 2 + [jax.ShapeDtypeStruct((side, side, 2, drows, D), BF16)]


def whole(n, arrays):
    g, u, d = arrays
    return g.reshape(-1, g.shape[-1]), u.reshape(-1, u.shape[-1]), d.reshape(-1, d.shape[-1])


def gather(n, wg, wu, wd, cid):
    L, rows, F = wg.shape
    drows, D = wd.shape[1:]
    layers = 2
    half = F // 2
    count = 2 + 4 * layers * COPIES

    def kernel(wg, wu, wd, *rest):
        outs = rest[:3], rest[3:6]
        praw, blk, send, recv, local = rest[6:]
        place = Place(n)
        c = place.c
        place.greet()
        sems = Sems(send, recv)
        raws = [sems.copy(w, praw.at[1, j], place.partner) for j, w in enumerate((wg, wu))]
        loads = [pltpu.make_async_copy(w, praw.at[0, j], local.at[j]) for j, w in enumerate((wg, wu))]
        flows, copies = [], []
        for l in range(layers):
            owns = [wd.at[l, pl.ds(lo, m)] for lo, m in down_split(drows)] + [blk.at[j, l] for j in (0, 1)]
            some, mine = gather_flows(place, sems, outs[l], owns)
            flows.append(some)
            copies.append([pltpu.make_async_copy(o, m, local.at[2 + 4 * l + k]) for k, (o, m) in enumerate(zip(owns, mine, strict=True))])

        def each(l, step, picked=slice(None)):
            for flow in flows[l][picked]:
                getattr(flow, step)()

        for copy in raws + loads + copies[0][:2] + copies[1][:2]:
            copy.start()
        each(0, "a1", slice(0, 2))
        for j in (0, 1):
            loads[j].wait()
            raws[j].wait_recv()
            for l in range(layers):
                for cc in (0, 1):
                    @pl.when(c == cc)
                    def _(cc=cc, j=j, l=l):
                        cols = slice(cc * half, (cc + 1) * half)
                        both = (praw[0, j, l, :, cols].astype(F32), praw[1, j, l, :, cols].astype(F32))
                        blk[j, l] = jnp.concatenate(both if cc == 0 else both[::-1], axis=0).astype(BF16)
        for copy in copies[0][2:] + copies[1][2:]:
            copy.start()
        each(0, "a1", slice(2, 4))
        each(0, "a2")
        for copy in copies[0]:
            copy.wait()
        each(0, "b1")
        each(1, "a1")
        each(0, "b2")
        each(1, "a2")
        each(0, "c1")
        each(0, "end")
        each(1, "got_a")
        for copy in copies[1]:
            copy.wait()
        for copy in raws:
            copy.wait_send()
        for flow in flows[0]:
            flow.sends(True)
            flow.sends(False)
        for flow in flows[1]:
            flow.sends(True)

    out = pl.pallas_call(
        kernel,
        out_shape=gather_shapes(n, rows, F, drows, D) * layers,
        in_specs=[pl.BlockSpec(memory_space=pltpu.HBM)] * 3,
        out_specs=[pl.BlockSpec(memory_space=pltpu.HBM)] * 6,
        scratch_shapes=[
            pltpu.VMEM((2, 2, L, rows, F), BF16),
            pltpu.VMEM((2, layers, 2 * rows, half), BF16),
            pltpu.SemaphoreType.DMA((count,)),
            pltpu.SemaphoreType.DMA((count,)),
            pltpu.SemaphoreType.DMA((2 + 4 * layers,)),
        ],
        compiler_params=pltpu.CompilerParams(collective_id=cid, has_side_effects=True, vmem_limit_bytes=60 << 20),
        name="gather",
    )(wg, wu, wd)
    return out[:3], out[3:]


class Scatter:
    def __init__(self, place, sems, axis, own, l1, part_a, full_a, total, snd_b, part_b, full_b):
        self.place, self.sems, self.axis = place, sems, axis
        self.own, self.l1, self.part_a, self.full_a, self.total, self.snd_b, self.part_b, self.full_b = (
            own, l1, part_a, full_a, total, snd_b, part_b, full_b)
        self.w = own.shape[-1]
        n, other = place.side, 1 - axis
        far_a, far_b = place.at(axis, 2), place.at(other, 2)
        self.sent_a, self.fwd_a, self.sent_b, self.fwd_b = [], [], [], []
        for h, (d, part) in enumerate(zip((1, -1), halves(self.w), strict=True)):
            run = pl.ds(h * (n // 2), n // 2)
            self.sent_a.append(sems.copy(own.at[order(axis, far_a, run)], part_a.at[h], place.hop(axis, d)))
            to = place.at(axis, d)
            self.fwd_a.append(sems.copy(own.at[order(axis, to, pl.ds(0, n))], full_a.at[h], place.hop(axis, d)))
            lanes = pl.ds(*part)
            self.sent_b.append(sems.copy(snd_b.at[far_b, :, lanes], part_b.at[h, :, lanes], place.hop(other, d)))
            self.fwd_b.append(sems.copy(snd_b.at[place.at(other, d)], full_b.at[h], place.hop(other, d)))

    def idx(self, a, b):
        return order(self.axis, a, b)

    def pair(self, a, b):
        i = self.idx(a, b)
        return self.own[i].astype(F32) + self.l1[i].astype(F32)

    def loop(self, lo, n, body):
        lax.fori_loop(lo, lo + n, lambda j, _: (body(j), 0)[1], 0)

    def a1(self):
        n = self.place.side
        far = self.place.at(self.axis, 2)

        def body(j):
            self.own[self.idx(far, j)] = self.pair(far, j).astype(BF16)

        self.loop(0, n, body)
        for copy in self.sent_a:
            copy.start()

    def a2(self):
        n = self.place.side
        for h, d in enumerate((1, -1)):
            to = self.place.at(self.axis, d)
            lo, rest = h * (n // 2), (1 - h) * (n // 2)

            def plain(j, to=to):
                self.own[self.idx(to, j)] = self.pair(to, j).astype(BF16)

            self.loop(rest, n // 2, plain)
            self.sent_a[h].wait_recv()

            def added(j, to=to, h=h, lo=lo):
                self.own[self.idx(to, j)] = (self.pair(to, j) + self.part_a[h, j - lo].astype(F32)).astype(BF16)

            self.loop(lo, n // 2, added)
            self.fwd_a[h].start()

    def b1(self):
        n = self.place.side
        p = self.place.at(self.axis, 0)
        for copy in self.fwd_a:
            copy.wait_recv()

        def body(j):
            self.total[j] = self.pair(p, j) + self.full_a[0, j].astype(F32) + self.full_a[1, j].astype(F32)

        self.loop(0, n, body)
        far = self.place.at(1 - self.axis, 2)
        self.snd_b[far] = self.total[far].astype(BF16)
        for copy in self.sent_b:
            copy.start()

    def b2(self):
        for h, (d, part) in enumerate(zip((1, -1), halves(self.w), strict=True)):
            to = self.place.at(1 - self.axis, d)
            lo, w = part
            rest = slice(w, self.w) if lo == 0 else slice(0, lo)
            got = slice(lo, lo + w)
            self.snd_b[to, :, rest] = self.total[to, :, rest].astype(BF16)
            self.sent_b[h].wait_recv()
            self.snd_b[to, :, got] = (self.total[to, :, got] + self.part_b[h, :, got].astype(F32)).astype(BF16)
            self.fwd_b[h].start()

    def last(self):
        for copy in self.fwd_b:
            copy.wait_recv()
        return self.total[self.place.at(1 - self.axis, 0)] + self.full_b[0].astype(F32) + self.full_b[1].astype(F32)


def scatter_scratch(side, r, w):
    return [
        pltpu.VMEM((side, side, r, w), BF16),
        pltpu.VMEM((side, side, r, w), BF16),
        pltpu.VMEM((2, side // 2, r, w), BF16),
        pltpu.VMEM((2, side, r, w), BF16),
        pltpu.VMEM((side, r, w), F32),
        pltpu.VMEM((side, r, w), BF16),
        pltpu.VMEM((2, r, w), BF16),
        pltpu.VMEM((2, r, w), BF16),
    ]


def scatter_phases(place, send, recv, local, terms, outs, swap, bufs):
    c = place.c
    sems = Sems(send, recv)
    down = len(terms) == 1
    half = terms[0].shape[-1] // 2

    def share(who):
        if down:
            return [terms[0].at[:, :, who, pl.ds(lo, m), :] for lo, m in down_split(terms[0].shape[3])]
        lanes = pl.ds(pl.multiple_of(who * half, 128), half)
        return [term.at[:, :, :, lanes] for term in terms]

    flows = [Scatter(place, sems, axis, *buf) for axis, buf in enumerate(bufs)]
    first = [sems.copy(theirs, flow.l1, place.partner) for theirs, flow in zip(share(1 - c), flows, strict=True)]
    loads = [pltpu.make_async_copy(mine, flow.own, local.at[k]) for k, (mine, flow) in enumerate(zip(share(c), flows, strict=True))]
    swaps = [] if down else [sems.copy(swap.at[0, j], swap.at[1, j], place.partner) for j in (0, 1)]

    def p0():
        for copy in first + loads:
            copy.start()

    def a1():
        for flow, got, load in zip(flows, first, loads, strict=True):
            load.wait()
            got.wait_recv()
            flow.a1()

    def every(step):
        def run():
            for flow in flows:
                getattr(flow, step)()
        return run

    def end():
        if down:
            for (lo, m), flow in zip(down_split(terms[0].shape[3]), flows, strict=True):
                outs[0][pl.ds(lo, m), :] = flow.last().astype(BF16)
        else:
            rows = outs[0].shape[0]
            for j in (0, 1):
                block = flows[j].last()
                parts = (block[:rows].astype(BF16), block[rows:].astype(BF16))
                for cc in (0, 1):
                    @pl.when(c == cc)
                    def _(cc=cc, parts=parts, j=j):
                        outs[j][:, cc * half : (cc + 1) * half] = parts[cc]
                        swap[0, j] = parts[1 - cc]
                swaps[j].start()
            for j, copy in enumerate(swaps):
                copy.wait_recv()
                for cc in (0, 1):
                    @pl.when(c == cc)
                    def _(cc=cc, j=j):
                        outs[j][:, (1 - cc) * half : (2 - cc) * half] = swap[1, j]
        sems.finish()

    return [p0, a1, every("a2"), every("b1"), every("b2"), end]


def scatter_parts(n, terms):
    side = math.isqrt(n // 2)
    R, W = terms[0].shape
    rows = R // n
    if len(terms) == 1:
        shapes = [(m, W) for _, m in down_split(rows)]
        operands = [terms[0].reshape(side, side, 2, rows, W)]
    else:
        shapes = [(2 * rows, W // 2)] * 2
        operands = [term.reshape(side, side, 2 * rows, W) for term in terms]
    groups = [scatter_scratch(side, r, w) for r, w in shapes]
    count = 2 * 9 + 2
    outs = [jax.ShapeDtypeStruct((rows, W), BF16)] * len(terms)
    scratch = [
        pltpu.VMEM((2, 2, rows, W // 2), BF16),
        pltpu.SemaphoreType.DMA((count,)),
        pltpu.SemaphoreType.DMA((count,)),
        pltpu.SemaphoreType.DMA((2,)),
    ] + [s for group in groups for s in group]
    return operands, outs, [pl.BlockSpec(memory_space=pltpu.VMEM)] * len(terms), scratch, len(groups[0])


class Beside:
    def __init__(self, n, terms, when, cid):
        self.n, self.when, self.on = n, when, terms is not None
        self.operands, self.outs, self.out_specs, self.scratch, self.kind = [], [], [], [], {}
        if self.on:
            self.operands, self.outs, self.out_specs, self.scratch, self.each = scatter_parts(n, terms)
            self.kind = {"collective_id": cid, "has_side_effects": True}

    def start(self, step, steps, terms, outs, scratch):
        if not self.on:
            return lambda: None
        place = Place(self.n)
        pl.when(step == 0)(place.greet)
        swap, send, recv, local, *flat = scratch
        bufs = [flat[i * self.each : (i + 1) * self.each] for i in range(2)]
        phases = scatter_phases(place, send, recv, local, terms, outs, swap, bufs)
        for phase, k in zip(phases, self.when, strict=True):
            if k < steps:
                pl.when(step == k)(phase)

        def rest():
            @pl.when(step == steps - 1)
            def _():
                for phase, k in zip(phases, self.when, strict=True):
                    if k >= steps:
                        phase()

        return rest


def dot(a, b, dims=((1,), (0,))):
    return lax.dot_general(a, b, (dims, ((), ())), preferred_element_type=F32)


ROWS_ROWS, COLS_COLS = ((0,), (0,)), ((1,), (1,))


def sigmoid(t):
    return 0.5 * jnp.tanh(0.5 * t) + 0.5


def scale_of(wide):
    return lax.rsqrt(jnp.mean(wide * wide, -1, keepdims=True) + 1e-6)


def normed(h):
    wide = h.astype(F32)
    return (wide * scale_of(wide)).astype(BF16)


def cut(n, most):
    return max(c for c in range(256, most + 1, 256) if n % c == 0)


HBM = pl.BlockSpec(memory_space=pltpu.HBM)
LIMIT = 62 << 20
TILE = {
    "f_t": 256, "f_c": 2560, "f_when": (5, 7),
    "b_t": 256, "b_c": 2560, "b_when": (0, 2, 4, 7, 8, 8),
    "s_t": 256, "s_c": 2560, "s_when": (0, 3, 6, 8, 8, 8),
    "d_c": 768,
    "g_c": 768, "g_when": (0, 1, 3, 5, 6, 6),
}


def once(shape, index):
    return pl.BlockSpec(shape, index, pipeline_mode=pl.Buffered(1))


def weight_spec(shape, index, pieces):
    return once(shape, index) if pieces == 1 else pl.BlockSpec(shape, index)


def forward(n, h, wg, wu, wd, nexts, cid):
    S, D = h.shape
    F = wg.shape[1]
    T, C = cut(S, TILE["f_t"]), cut(F, TILE["f_c"])
    nt, nc = S // T, F // C
    steps = nt * nc
    when = TILE["f_when"]
    count = 4 * COPIES

    def kernel(h, wg, wu, wd, ig, iu, id_, o, og, ou, od, a, acc, send, recv):
        j = pl.program_id(1)
        step = pl.program_id(0) * nc + j
        place = Place(n)
        pl.when(step == 0)(place.greet)
        flows, _ = gather_flows(place, Sems(send, recv), (og, ou, od), None)

        def every(what):
            def run():
                for flow in flows:
                    getattr(flow, what)()
            return run

        pl.when(step == 0)(every("b1_next"))
        pl.when(step == when[0])(every("b2"))
        pl.when(step == when[1])(every("c1"))

        @pl.when(j == 0)
        def _():
            a[...] = normed(h[...])
            acc[...] = jnp.zeros_like(acc)

        gate, up = dot(a[...], wg[...]), dot(a[...], wu[...])
        act = (gate * sigmoid(gate) * up).astype(BF16)
        acc[...] += dot(act, wd[...])

        @pl.when(j == nc - 1)
        def _():
            o[...] = (h[...].astype(F32) + acc[...].astype(BF16).astype(F32)).astype(BF16)

        @pl.when(step == steps - 1)
        def _():
            every("end")()
            for flow in flows:
                flow.sends(False)

    out = pl.pallas_call(
        kernel,
        grid=(nt, nc),
        out_shape=[jax.ShapeDtypeStruct((S, D), BF16)] + [jax.ShapeDtypeStruct(t.shape, BF16) for t in nexts],
        in_specs=[
            pl.BlockSpec((T, D), lambda i, j: (i, 0)),
            weight_spec((D, C), lambda i, j: (0, j), nc),
            weight_spec((D, C), lambda i, j: (0, j), nc),
            weight_spec((C, D), lambda i, j: (j, 0), nc),
            HBM,
            HBM,
            HBM,
        ],
        out_specs=[pl.BlockSpec((T, D), lambda i, j: (i, 0)), HBM, HBM, HBM],
        scratch_shapes=[
            pltpu.VMEM((T, D), BF16),
            pltpu.VMEM((T, D), F32),
            pltpu.SemaphoreType.DMA((count,)),
            pltpu.SemaphoreType.DMA((count,)),
        ],
        input_output_aliases={4: 1, 5: 2, 6: 3},
        compiler_params=pltpu.CompilerParams(
            collective_id=cid, has_side_effects=True, vmem_limit_bytes=LIMIT, dimension_semantics=("arbitrary", "arbitrary")
        ),
        cost_estimate=pl.CostEstimate(flops=6 * S * D * F, bytes_accessed=4 * S * D, transcendentals=S * F),
        name="forward",
    )(h, wg, wu, wd, *nexts)
    return out[0], out[1:]


def by_normed(h, by_a, dy):
    by_a = by_a.astype(BF16).astype(F32)
    wide = h.astype(F32)
    scale = scale_of(wide)
    hat = wide * scale
    by_wide = scale * (by_a - hat * jnp.mean(by_a * hat, -1, keepdims=True))
    return (dy.astype(F32) + by_wide.astype(BF16).astype(F32)).astype(BF16)


def backward(n, h, dy, wg, wu, wd, full, terms, cid):
    S, D = h.shape
    F = wg.shape[1]
    T, C = cut(S, TILE["b_t"]), cut(F, TILE["b_c"])
    nt, nc = S // T, F // C
    steps = nt * nc
    beside = Beside(n, terms, TILE["b_when"], cid)
    most = 5 if full else 4

    def kernel(h, dy, wg, wu, wd, *rest):
        k = len(beside.operands)
        terms_, rest = rest[:k], rest[k:]
        (act, dg, du, a), dh, rest = rest[:4], rest[most - 1], rest[most:]
        k = len(beside.outs)
        sums, rest = rest[:k], rest[k:]
        acc, rest = (rest[0], rest[1:]) if full else (None, rest)
        j = pl.program_id(1)
        step = pl.program_id(0) * nc + j
        left = beside.start(step, steps, terms_, sums, rest)

        @pl.when(j == 0)
        def _():
            a[...] = normed(h[...])
            if full:
                acc[...] = jnp.zeros_like(acc)

        gate, up = dot(a[...], wg[...]), dot(a[...], wu[...])
        dact = dot(dy[...], wd[...], COLS_COLS).astype(BF16).astype(F32)
        sig = sigmoid(gate)
        silu = gate * sig
        act[...] = (silu * up).astype(BF16)
        by_up = (dact * silu).astype(BF16)
        by_gate = (dact * up * (sig + silu * (1.0 - sig))).astype(BF16)
        du[...] = by_up
        dg[...] = by_gate
        if full:
            acc[...] += dot(by_gate, wg[...], COLS_COLS) + dot(by_up, wu[...], COLS_COLS)

            @pl.when(j == nc - 1)
            def _():
                dh[...] = by_normed(h[...], acc[...], dy[...])

        left()

    tile = pl.BlockSpec((T, D), lambda i, j: (i, 0))
    wide_tile = pl.BlockSpec((T, C), lambda i, j: (i, j))
    out = pl.pallas_call(
        kernel,
        grid=(nt, nc),
        out_shape=[jax.ShapeDtypeStruct((S, F), BF16)] * 3 + [jax.ShapeDtypeStruct((S, D), BF16)] * (most - 3) + beside.outs,
        in_specs=[
            tile,
            tile,
            weight_spec((D, C), lambda i, j: (0, j), nc),
            weight_spec((D, C), lambda i, j: (0, j), nc),
            weight_spec((C, D), lambda i, j: (j, 0), nc),
        ]
        + [HBM] * len(beside.operands),
        out_specs=[wide_tile] * 3 + [tile] * (most - 3) + beside.out_specs,
        scratch_shapes=[pltpu.VMEM((T, D), F32)] * full + beside.scratch,
        compiler_params=pltpu.CompilerParams(vmem_limit_bytes=LIMIT, dimension_semantics=("arbitrary", "arbitrary"), **beside.kind),
        cost_estimate=pl.CostEstimate(flops=10 * S * D * F, bytes_accessed=6 * S * F, transcendentals=S * F),
        name=f"backward{cid}",
    )(h, dy, wg, wu, wd, *beside.operands)
    return out[:most], out[most:]


def to_state(n, h, dy, dg, du, wg, wu, terms, cid):
    S, D = h.shape
    F = wg.shape[1]
    T, C = cut(S, TILE["s_t"]), cut(F, TILE["s_c"])
    nt, nc = S // T, F // C
    steps = nt * nc
    beside = Beside(n, terms, TILE["s_when"], cid)

    def kernel(h, dy, dg, du, wg, wu, *rest):
        k = len(beside.operands)
        terms_, dh, rest = rest[:k], rest[k], rest[k + 1 :]
        k = len(beside.outs)
        sums, acc, rest = rest[:k], rest[k], rest[k + 1 :]
        j = pl.program_id(1)
        step = pl.program_id(0) * nc + j
        left = beside.start(step, steps, terms_, sums, rest)

        @pl.when(j == 0)
        def _():
            acc[...] = jnp.zeros_like(acc)

        acc[...] += dot(dg[...], wg[...], COLS_COLS) + dot(du[...], wu[...], COLS_COLS)

        @pl.when(j == nc - 1)
        def _():
            dh[...] = by_normed(h[...], acc[...], dy[...])

        left()

    tile = pl.BlockSpec((T, D), lambda i, j: (i, 0))
    wide_tile = pl.BlockSpec((T, C), lambda i, j: (i, j))
    weight = weight_spec((D, C), lambda i, j: (0, j), nc)
    out = pl.pallas_call(
        kernel,
        grid=(nt, nc),
        out_shape=[jax.ShapeDtypeStruct((S, D), BF16)] + beside.outs,
        in_specs=[tile, tile, wide_tile, wide_tile, weight, weight] + [HBM] * len(beside.operands),
        out_specs=[tile] + beside.out_specs,
        scratch_shapes=[pltpu.VMEM((T, D), F32)] + beside.scratch,
        compiler_params=pltpu.CompilerParams(vmem_limit_bytes=LIMIT, dimension_semantics=("arbitrary", "arbitrary"), **beside.kind),
        cost_estimate=pl.CostEstimate(flops=4 * S * D * F, bytes_accessed=4 * S * F, transcendentals=0),
        name="to_state",
    )(h, dy, dg, du, wg, wu, *beside.operands)
    return out[0], out[1:]


def down_weight(act, dy):
    S, D = dy.shape
    F = act.shape[1]
    C = cut(F, TILE["d_c"])

    def kernel(act, dy, od):
        od[...] = dot(act[...], dy[...], ROWS_ROWS).astype(BF16)

    return pl.pallas_call(
        kernel,
        grid=(F // C,),
        out_shape=jax.ShapeDtypeStruct((F, D), BF16),
        in_specs=[pl.BlockSpec((S, C), lambda i: (0, i)), once((S, D), lambda i: (0, 0))],
        out_specs=pl.BlockSpec((C, D), lambda i: (i, 0)),
        compiler_params=pltpu.CompilerParams(vmem_limit_bytes=LIMIT, dimension_semantics=("arbitrary",)),
        cost_estimate=pl.CostEstimate(flops=2 * S * D * F, bytes_accessed=2 * S * F, transcendentals=0),
        name="down_weight",
    )(act, dy)


def gate_weights(n, a, dg, du, terms, cid):
    S, D = a.shape
    F = dg.shape[1]
    C = cut(F, TILE["g_c"])
    nc = F // C
    steps = 2 * nc
    beside = Beside(n, terms, TILE["g_when"], cid)

    def kernel(a, dg, du, *rest):
        k = len(beside.operands)
        terms_, og, ou, rest = rest[:k], rest[k], rest[k + 1], rest[k + 2 :]
        k = len(beside.outs)
        sums, rest = rest[:k], rest[k:]
        step = pl.program_id(0)
        left = beside.start(step, steps, terms_, sums, rest)

        @pl.when(step < nc)
        def _():
            og[...] = dot(a[...], dg[...], ROWS_ROWS).astype(BF16)

        @pl.when(step >= nc)
        def _():
            ou[...] = dot(a[...], du[...], ROWS_ROWS).astype(BF16)

        left()

    def cols(k, rows):
        return pl.BlockSpec((rows, C), lambda i: (0, jnp.clip(i - k * nc, 0, nc - 1)))

    out = pl.pallas_call(
        kernel,
        grid=(steps,),
        out_shape=[jax.ShapeDtypeStruct((D, F), BF16)] * 2 + beside.outs,
        in_specs=[once((S, D), lambda i: (0, 0)), cols(0, S), cols(1, S)] + [HBM] * len(beside.operands),
        out_specs=[cols(0, D), cols(1, D)] + beside.out_specs,
        scratch_shapes=beside.scratch,
        compiler_params=pltpu.CompilerParams(vmem_limit_bytes=LIMIT, dimension_semantics=("arbitrary",), **beside.kind),
        cost_estimate=pl.CostEstimate(flops=4 * S * D * F, bytes_accessed=4 * S * F, transcendentals=0),
        name=f"gate_weights{cid}",
    )(a, dg, du, *beside.operands)
    return out[:2], out[2:]


def solution(mesh):
    n = mesh.shape["dp"]

    def device(x, dy, wg, wu, wd):
        x, dy = x.reshape(x.shape[1:]), dy.reshape(dy.shape[1:])
        first, nexts = gather(n, wg, wu, wd, 0)
        w0 = whole(n, first)
        h, second = forward(n, x, *w0, nexts, 1)
        w1 = whole(n, second)

        (act, dg, du, a, dh), _ = backward(n, h, dy, *w1, True, None, 2)
        down = down_weight(act, dy)
        gates, (down1,) = gate_weights(n, a, dg, du, [down], 3)

        (act, dg, du, a), gates1 = backward(n, x, dh, *w0, False, gates, 4)
        down = down_weight(act, dh)
        gates, (down0,) = gate_weights(n, a, dg, du, [down], 5)
        dx, gates0 = to_state(n, x, dh, dg, du, *w0[:2], gates, 6)
        sums = [(*gates0, down0), (*gates1, down1)]
        return (dx[None], *(jnp.stack([s[j] for s in sums]) for j in range(3)))

    tokens, rows = P(("rep", "dp")), P(None, "dp")
    return jax.shard_map(
        device, mesh=mesh, in_specs=(tokens, tokens, rows, rows, rows), out_specs=(tokens, *[P("rep", "dp")] * 3), check_vma=False
    )
```

```python
import functools
import math
import jax
import jax.numpy as jnp
from jax import lax
from jax.experimental import pallas as pl
from jax.experimental.pallas import tpu as pltpu
from jax.sharding import PartitionSpec as P

MESH = pl.DeviceIdType.MESH
F32, BF16 = jnp.float32, jnp.bfloat16
ALL = slice(None)


def halves(n):
    first = (n // 128 + 1) // 2 * 128
    return (0, first), (first, n - first)


class Place:
    def __init__(self, n):
        self.side = math.isqrt(n // 2)
        me = lax.axis_index("dp")
        chip = me // 2
        self.c = me % 2
        self.xy = (chip // self.side, chip % self.side)
        self.partner = {"dp": chip * 2 + 1 - self.c}
        self.places = {(a, d): lax.rem(self.xy[a] + d + self.side, self.side) for a in (0, 1) for d in range(-2, 3)}
        self.hops = {}
        for a in (0, 1):
            for d in (1, -1):
                xy = list(self.xy)
                xy[a] = self.places[a, d]
                self.hops[a, d] = {"dp": (xy[0] * self.side + xy[1]) * 2 + self.c}

    def hop(self, axis, by):
        return self.hops[axis, by]

    def at(self, axis, by):
        return self.places[axis, by]

    def greet(self):
        barrier = pltpu.get_barrier_semaphore()
        others = [self.partner] + [self.hop(a, d) for a in (0, 1) for d in (1, -1)]
        for other in others:
            pl.semaphore_signal(barrier, inc=1, device_id=other, device_id_type=MESH)
        pl.semaphore_wait(barrier, len(others))


class Sems:
    def __init__(self, send, recv):
        self.send, self.recv, self.used, self.started = send, recv, 0, []

    def copy(self, src, dst, to):
        k = self.used
        self.used += 1
        made = pltpu.make_async_remote_copy(
            src_ref=src, dst_ref=dst, send_sem=self.send.at[k], recv_sem=self.recv.at[k], device_id=to, device_id_type=MESH
        )
        self.started.append(made)
        return made

    def finish(self):
        for made in self.started:
            made.wait_send()


def order(axis, a, b):
    return (a, b) if axis == 0 else (b, a)


class Gather:
    def __init__(self, place, sems, view, own, axis, lanes):
        n, other = place.side, 1 - axis
        p, q = place.at(axis, 0), place.at(other, 0)

        def slab(q, half=None):
            run = pl.ds(0, n) if half is None else pl.ds(half * (n // 2), n // 2)
            return view(*order(axis, run, q), None)

        self.sent_a, self.fwd_a, self.sent_b, self.fwd_b, self.swap = [], [], [], [], []
        mine = slab(q)
        self.swap.append(sems.copy(mine, mine, place.partner))
        for half, (d, part) in enumerate(zip((1, -1), halves(lanes), strict=True)):
            self.sent_a.append(sems.copy(own, view(*order(axis, p, q), None), place.hop(axis, d)))
            got = view(*order(axis, place.at(axis, -d), q), part)
            self.fwd_a.append(sems.copy(got, got, place.hop(axis, d)))
            self.sent_b.append(sems.copy(mine, mine, place.hop(other, d)))
            got = slab(place.at(other, -d), half)
            self.fwd_b.append(sems.copy(got, got, place.hop(other, d)))
            whole = slab(place.at(other, -d))
            self.swap.append(sems.copy(whole, whole, place.partner))
            got = slab(place.at(other, -2 * d), half)
            self.swap.append(sems.copy(got, got, place.partner))

    def a1(self):
        for copy in self.sent_a:
            copy.start()

    def a2(self):
        for k in (0, 1):
            self.sent_a[k].wait_recv()
            self.fwd_a[k].start()

    def b1(self):
        for copy in self.fwd_a:
            copy.wait_recv()
        for copy in self.sent_b:
            copy.start()
        self.swap[0].start()

    def b2(self):
        for k in (0, 1):
            self.sent_b[k].wait_recv()
            self.fwd_b[k].start()
            self.swap[1 + 2 * k].start()

    def c1(self):
        for k in (0, 1):
            self.fwd_b[k].wait_recv()
            self.swap[2 + 2 * k].start()

    def end(self):
        for copy in self.swap:
            copy.wait_recv()

    def got_a(self):
        for copy in self.fwd_a:
            copy.wait_recv()

    def b1_next(self):
        for copy in self.sent_b:
            copy.start()
        self.swap[0].start()

    def sends(self, first):
        for copy in self.sent_a + self.fwd_a if first else self.sent_b + self.fwd_b + self.swap:
            copy.wait_send()


def down_split(drows):
    first = (drows // 8 + 1) // 2 * 8
    return ((0, first), (first, drows - first))


COPIES = 13


def gather_flows(place, sems, outs, owns):
    c = place.c
    half = outs[0].shape[-1] // 2
    D = outs[2].shape[-1]
    flows, views = [], []
    for j, (lo, m) in enumerate(down_split(outs[2].shape[3])):
        def view(xs, ys, part, lo=lo, m=m):
            return outs[2].at[xs, ys, c, pl.ds(lo, m), ALL if part is None else pl.ds(*part)]
        views.append((view, j, D))
    for j in (0, 1):
        def view(xs, ys, part, j=j):
            lo, m = (0, half) if part is None else part
            return outs[j].at[xs, ys, :, pl.ds(pl.multiple_of(c * half + lo, 128), m)]
        views.append((view, j, half))
    mine = [view(*place.xy, None) for view, _, _ in views]
    flows = [Gather(place, sems, view, own, axis, lanes) for (view, axis, lanes), own in zip(views, owns or mine, strict=True)]
    return flows, mine


def gather_shapes(n, rows, F, drows, D):
    side = math.isqrt(n // 2)
    return [jax.ShapeDtypeStruct((side, side, 2 * rows, F), BF16)] * 2 + [jax.ShapeDtypeStruct((side, side, 2, drows, D), BF16)]


def whole(n, arrays):
    g, u, d = arrays
    return g.reshape(-1, g.shape[-1]), u.reshape(-1, u.shape[-1]), d.reshape(-1, d.shape[-1])


def gather(n, wg, wu, wd, cid):
    L, rows, F = wg.shape
    drows, D = wd.shape[1:]
    layers = 2
    half = F // 2
    count = 2 + 4 * layers * COPIES

    def kernel(wg, wu, wd, *rest):
        outs = rest[:3], rest[3:6]
        praw, blk, send, recv, local = rest[6:]
        place = Place(n)
        c = place.c
        place.greet()
        sems = Sems(send, recv)
        raws = [sems.copy(w, praw.at[1, j], place.partner) for j, w in enumerate((wg, wu))]
        loads = [pltpu.make_async_copy(w, praw.at[0, j], local.at[j]) for j, w in enumerate((wg, wu))]
        flows, copies = [], []
        for l in range(layers):
            owns = [wd.at[l, pl.ds(lo, m)] for lo, m in down_split(drows)] + [blk.at[j, l] for j in (0, 1)]
            some, mine = gather_flows(place, sems, outs[l], owns)
            flows.append(some)
            copies.append([pltpu.make_async_copy(o, m, local.at[2 + 4 * l + k]) for k, (o, m) in enumerate(zip(owns, mine, strict=True))])

        def each(l, step, picked=slice(None)):
            for flow in flows[l][picked]:
                getattr(flow, step)()

        for copy in raws + loads + copies[0][:2] + copies[1][:2]:
            copy.start()
        each(0, "a1", slice(0, 2))
        for j in (0, 1):
            loads[j].wait()
            raws[j].wait_recv()
            for l in range(layers):
                for cc in (0, 1):
                    @pl.when(c == cc)
                    def _(cc=cc, j=j, l=l):
                        cols = slice(cc * half, (cc + 1) * half)
                        both = (praw[0, j, l, :, cols].astype(F32), praw[1, j, l, :, cols].astype(F32))
                        blk[j, l] = jnp.concatenate(both if cc == 0 else both[::-1], axis=0).astype(BF16)
        for copy in copies[0][2:] + copies[1][2:]:
            copy.start()
        each(0, "a1", slice(2, 4))
        each(0, "a2")
        for copy in copies[0]:
            copy.wait()
        each(0, "b1")
        each(1, "a1")
        each(0, "b2")
        each(1, "a2")
        each(0, "c1")
        each(0, "end")
        each(1, "got_a")
        for copy in copies[1]:
            copy.wait()
        for copy in raws:
            copy.wait_send()
        for flow in flows[0]:
            flow.sends(True)
            flow.sends(False)
        for flow in flows[1]:
            flow.sends(True)

    out = pl.pallas_call(
        kernel,
        out_shape=gather_shapes(n, rows, F, drows, D) * layers,
        in_specs=[pl.BlockSpec(memory_space=pltpu.HBM)] * 3,
        out_specs=[pl.BlockSpec(memory_space=pltpu.HBM)] * 6,
        scratch_shapes=[
            pltpu.VMEM((2, 2, L, rows, F), BF16),
            pltpu.VMEM((2, layers, 2 * rows, half), BF16),
            pltpu.SemaphoreType.DMA((count,)),
            pltpu.SemaphoreType.DMA((count,)),
            pltpu.SemaphoreType.DMA((2 + 4 * layers,)),
        ],
        compiler_params=pltpu.CompilerParams(collective_id=cid, has_side_effects=True, vmem_limit_bytes=60 << 20),
        name="gather",
    )(wg, wu, wd)
    return out[:3], out[3:]


class Scatter:
    def __init__(self, place, sems, axis, own, l1, part_a, full_a, total, snd_b, part_b, full_b):
        self.place, self.sems, self.axis = place, sems, axis
        self.own, self.l1, self.part_a, self.full_a, self.total, self.snd_b, self.part_b, self.full_b = (
            own, l1, part_a, full_a, total, snd_b, part_b, full_b)
        self.w = own.shape[-1]
        n, other = place.side, 1 - axis
        far_a, far_b = place.at(axis, 2), place.at(other, 2)
        self.sent_a, self.fwd_a, self.sent_b, self.fwd_b = [], [], [], []
        for h, (d, part) in enumerate(zip((1, -1), halves(self.w), strict=True)):
            run = pl.ds(h * (n // 2), n // 2)
            self.sent_a.append(sems.copy(own.at[order(axis, far_a, run)], part_a.at[h], place.hop(axis, d)))
            to = place.at(axis, d)
            self.fwd_a.append(sems.copy(own.at[order(axis, to, pl.ds(0, n))], full_a.at[h], place.hop(axis, d)))
            lanes = pl.ds(*part)
            self.sent_b.append(sems.copy(snd_b.at[far_b, :, lanes], part_b.at[h, :, lanes], place.hop(other, d)))
            self.fwd_b.append(sems.copy(snd_b.at[place.at(other, d)], full_b.at[h], place.hop(other, d)))

    def idx(self, a, b):
        return order(self.axis, a, b)

    def pair(self, a, b):
        i = self.idx(a, b)
        return self.own[i].astype(F32) + self.l1[i].astype(F32)

    def loop(self, lo, n, body):
        lax.fori_loop(lo, lo + n, lambda j, _: (body(j), 0)[1], 0)

    def a1(self):
        n = self.place.side
        far = self.place.at(self.axis, 2)

        def body(j):
            self.own[self.idx(far, j)] = self.pair(far, j).astype(BF16)

        self.loop(0, n, body)
        for copy in self.sent_a:
            copy.start()

    def a2(self):
        n = self.place.side
        for h, d in enumerate((1, -1)):
            to = self.place.at(self.axis, d)
            lo, rest = h * (n // 2), (1 - h) * (n // 2)

            def plain(j, to=to):
                self.own[self.idx(to, j)] = self.pair(to, j).astype(BF16)

            self.loop(rest, n // 2, plain)
            self.sent_a[h].wait_recv()

            def added(j, to=to, h=h, lo=lo):
                self.own[self.idx(to, j)] = (self.pair(to, j) + self.part_a[h, j - lo].astype(F32)).astype(BF16)

            self.loop(lo, n // 2, added)
            self.fwd_a[h].start()

    def b1(self):
        n = self.place.side
        p = self.place.at(self.axis, 0)
        for copy in self.fwd_a:
            copy.wait_recv()

        def body(j):
            self.total[j] = self.pair(p, j) + self.full_a[0, j].astype(F32) + self.full_a[1, j].astype(F32)

        self.loop(0, n, body)
        far = self.place.at(1 - self.axis, 2)
        self.snd_b[far] = self.total[far].astype(BF16)
        for copy in self.sent_b:
            copy.start()

    def b2(self):
        for h, (d, part) in enumerate(zip((1, -1), halves(self.w), strict=True)):
            to = self.place.at(1 - self.axis, d)
            lo, w = part
            rest = slice(w, self.w) if lo == 0 else slice(0, lo)
            got = slice(lo, lo + w)
            self.snd_b[to, :, rest] = self.total[to, :, rest].astype(BF16)
            self.sent_b[h].wait_recv()
            self.snd_b[to, :, got] = (self.total[to, :, got] + self.part_b[h, :, got].astype(F32)).astype(BF16)
            self.fwd_b[h].start()

    def last(self):
        for copy in self.fwd_b:
            copy.wait_recv()
        return self.total[self.place.at(1 - self.axis, 0)] + self.full_b[0].astype(F32) + self.full_b[1].astype(F32)


def scatter_scratch(side, r, w):
    return [
        pltpu.VMEM((side, side, r, w), BF16),
        pltpu.VMEM((side, side, r, w), BF16),
        pltpu.VMEM((2, side // 2, r, w), BF16),
        pltpu.VMEM((2, side, r, w), BF16),
        pltpu.VMEM((side, r, w), F32),
        pltpu.VMEM((side, r, w), BF16),
        pltpu.VMEM((2, r, w), BF16),
        pltpu.VMEM((2, r, w), BF16),
    ]


def scatter_phases(place, send, recv, local, terms, outs, swap, bufs):
    c = place.c
    sems = Sems(send, recv)
    terms = terms[0]
    down = len(outs) == 1
    half = terms.shape[-1] // 2

    def share(who):
        if down:
            return [terms.at[:, :, who, pl.ds(lo, m), :] for lo, m in down_split(terms.shape[3])]
        lanes = pl.ds(pl.multiple_of(who * half, 128), half)
        return [terms.at[j, :, :, :, lanes] for j in (0, 1)]

    flows = [Scatter(place, sems, axis, *buf) for axis, buf in enumerate(bufs)]
    first = [sems.copy(theirs, flow.l1, place.partner) for theirs, flow in zip(share(1 - c), flows, strict=True)]
    loads = [pltpu.make_async_copy(mine, flow.own, local.at[k]) for k, (mine, flow) in enumerate(zip(share(c), flows, strict=True))]
    swaps = [] if down else [sems.copy(swap.at[0, j], swap.at[1, j], place.partner) for j in (0, 1)]

    def p0():
        for copy in first + loads:
            copy.start()

    def a1():
        for flow, got, load in zip(flows, first, loads, strict=True):
            load.wait()
            got.wait_recv()
            flow.a1()

    def every(step):
        def run():
            for flow in flows:
                getattr(flow, step)()
        return run

    def end():
        if down:
            for (lo, m), flow in zip(down_split(terms.shape[3]), flows, strict=True):
                outs[0][pl.ds(lo, m), :] = flow.last().astype(BF16)
        else:
            rows = outs[0].shape[0]
            for j in (0, 1):
                block = flows[j].last()
                parts = (block[:rows].astype(BF16), block[rows:].astype(BF16))
                for cc in (0, 1):
                    @pl.when(c == cc)
                    def _(cc=cc, parts=parts, j=j):
                        outs[j][:, cc * half : (cc + 1) * half] = parts[cc]
                        swap[0, j] = parts[1 - cc]
                swaps[j].start()
            for j, copy in enumerate(swaps):
                copy.wait_recv()
                for cc in (0, 1):
                    @pl.when(c == cc)
                    def _(cc=cc, j=j):
                        outs[j][:, (1 - cc) * half : (2 - cc) * half] = swap[1, j]
        sems.finish()

    return [p0, a1, every("a2"), every("b1"), every("b2"), end]


def scatter_parts(n, terms):
    side = math.isqrt(n // 2)
    R, W = terms.shape[-2:]
    rows = R // n
    if terms.ndim == 2:
        shapes = [(m, W) for _, m in down_split(rows)]
        operands = [terms.reshape(side, side, 2, rows, W)]
    else:
        shapes = [(2 * rows, W // 2)] * 2
        operands = [terms.reshape(2, side, side, 2 * rows, W)]
    groups = [scatter_scratch(side, r, w) for r, w in shapes]
    count = 2 * 9 + 2
    outs = [jax.ShapeDtypeStruct((rows, W), BF16)] * (terms.ndim - 1)
    scratch = [
        pltpu.VMEM((2, 2, rows, W // 2), BF16),
        pltpu.SemaphoreType.DMA((count,)),
        pltpu.SemaphoreType.DMA((count,)),
        pltpu.SemaphoreType.DMA((2,)),
    ] + [s for group in groups for s in group]
    return operands, outs, [pl.BlockSpec(memory_space=pltpu.VMEM)] * len(outs), scratch, len(groups[0])


class Beside:
    def __init__(self, n, terms, when, cid):
        self.n, self.when, self.on = n, when, terms is not None
        self.operands, self.outs, self.out_specs, self.scratch, self.kind = [], [], [], [], {}
        if self.on:
            self.operands, self.outs, self.out_specs, self.scratch, self.each = scatter_parts(n, terms)
            self.kind = {"collective_id": cid, "has_side_effects": True}

    def start(self, step, steps, terms, outs, scratch):
        if not self.on:
            return lambda: None
        place = Place(self.n)
        pl.when(step == 0)(place.greet)
        swap, send, recv, local, *flat = scratch
        bufs = [flat[i * self.each : (i + 1) * self.each] for i in range(2)]
        phases = scatter_phases(place, send, recv, local, terms, outs, swap, bufs)
        for phase, k in zip(phases, self.when, strict=True):
            if k < steps:
                pl.when(step == k)(phase)

        def rest():
            @pl.when(step == steps - 1)
            def _():
                for phase, k in zip(phases, self.when, strict=True):
                    if k >= steps:
                        phase()

        return rest


def dot(a, b, dims=((1,), (0,))):
    return lax.dot_general(a, b, (dims, ((), ())), preferred_element_type=F32)


ROWS_ROWS, COLS_COLS = ((0,), (0,)), ((1,), (1,))


def sigmoid(t):
    return 0.5 * jnp.tanh(0.5 * t) + 0.5


def scale_of(wide):
    return lax.rsqrt(jnp.mean(wide * wide, -1, keepdims=True) + 1e-6)


def normed(h):
    wide = h.astype(F32)
    return (wide * scale_of(wide)).astype(BF16)


def cut(n, most):
    return max(c for c in range(256, most + 1, 256) if n % c == 0)


HBM = pl.BlockSpec(memory_space=pltpu.HBM)
LIMIT = 62 << 20
TILE = {
    "f_t": 256, "f_c": 2560, "f_when": (4, 7),
    "b_t": 256, "b_c": 2560, "b_when": (0, 1, 3, 6, 7, 8),
    "s_t": 256, "s_c": 2560, "s_when": (0, 2, 4, 8, 8, 8),
    "d_c": 768,
    "g_c": 768, "g_when": (0, 1, 2, 4, 5, 6),
}


def once(shape, index):
    return pl.BlockSpec(shape, index, pipeline_mode=pl.Buffered(1))


def weight_spec(shape, index, pieces):
    return once(shape, index) if pieces == 1 else pl.BlockSpec(shape, index)


def forward(n, h, wg, wu, wd, nexts, cid):
    S, D = h.shape
    F = wg.shape[1]
    T, C = cut(S, TILE["f_t"]), cut(F, TILE["f_c"])
    nt, nc = S // T, F // C
    steps = nt * nc
    when = TILE["f_when"]
    count = 4 * COPIES

    def kernel(h, wg, wu, wd, ig, iu, id_, o, og, ou, od, a, acc, send, recv):
        j = pl.program_id(1)
        step = pl.program_id(0) * nc + j
        place = Place(n)
        pl.when(step == 0)(place.greet)
        flows, _ = gather_flows(place, Sems(send, recv), (og, ou, od), None)

        def every(what):
            def run():
                for flow in flows:
                    getattr(flow, what)()
            return run

        pl.when(step == 0)(every("b1_next"))
        pl.when(step == when[0])(every("b2"))
        pl.when(step == when[1])(every("c1"))

        @pl.when(j == 0)
        def _():
            a[...] = normed(h[...])
            acc[...] = jnp.zeros_like(acc)

        gate, up = dot(a[...], wg[...]), dot(a[...], wu[...])
        act = (gate * sigmoid(gate) * up).astype(BF16)
        acc[...] += dot(act, wd[...])

        @pl.when(j == nc - 1)
        def _():
            o[...] = (h[...].astype(F32) + acc[...].astype(BF16).astype(F32)).astype(BF16)

        @pl.when(step == steps - 1)
        def _():
            every("end")()
            for flow in flows:
                flow.sends(False)

    out = pl.pallas_call(
        kernel,
        grid=(nt, nc),
        out_shape=[jax.ShapeDtypeStruct((S, D), BF16)] + [jax.ShapeDtypeStruct(t.shape, BF16) for t in nexts],
        in_specs=[
            pl.BlockSpec((T, D), lambda i, j: (i, 0)),
            weight_spec((D, C), lambda i, j: (0, j), nc),
            weight_spec((D, C), lambda i, j: (0, j), nc),
            weight_spec((C, D), lambda i, j: (j, 0), nc),
            HBM,
            HBM,
            HBM,
        ],
        out_specs=[pl.BlockSpec((T, D), lambda i, j: (i, 0)), HBM, HBM, HBM],
        scratch_shapes=[
            pltpu.VMEM((T, D), BF16),
            pltpu.VMEM((T, D), F32),
            pltpu.SemaphoreType.DMA((count,)),
            pltpu.SemaphoreType.DMA((count,)),
        ],
        input_output_aliases={4: 1, 5: 2, 6: 3},
        compiler_params=pltpu.CompilerParams(
            collective_id=cid, has_side_effects=True, vmem_limit_bytes=LIMIT, dimension_semantics=("arbitrary", "arbitrary")
        ),
        cost_estimate=pl.CostEstimate(flops=6 * S * D * F, bytes_accessed=4 * S * D, transcendentals=S * F),
        name="forward",
    )(h, wg, wu, wd, *nexts)
    return out[0], out[1:]


def by_normed(h, by_a, dy):
    by_a = by_a.astype(BF16).astype(F32)
    wide = h.astype(F32)
    scale = scale_of(wide)
    hat = wide * scale
    by_wide = scale * (by_a - hat * jnp.mean(by_a * hat, -1, keepdims=True))
    return (dy.astype(F32) + by_wide.astype(BF16).astype(F32)).astype(BF16)


def backward(n, h, dy, wg, wu, wd, full, terms, cid):
    S, D = h.shape
    F = wg.shape[1]
    T, C = cut(S, TILE["b_t"]), cut(F, TILE["b_c"])
    nt, nc = S // T, F // C
    steps = nt * nc
    beside = Beside(n, terms, TILE["b_when"], cid)
    most = 4 if full else 3

    def kernel(h, dy, wg, wu, wd, *rest):
        k = len(beside.operands)
        terms_, rest = rest[:k], rest[k:]
        (act, dgu, a), dh, rest = rest[:3], rest[most - 1], rest[most:]
        k = len(beside.outs)
        sums, rest = rest[:k], rest[k:]
        acc, rest = (rest[0], rest[1:]) if full else (None, rest)
        j = pl.program_id(1)
        step = pl.program_id(0) * nc + j
        left = beside.start(step, steps, terms_, sums, rest)

        @pl.when(j == 0)
        def _():
            a[...] = normed(h[...])
            if full:
                acc[...] = jnp.zeros_like(acc)

        gate, up = dot(a[...], wg[...]), dot(a[...], wu[...])
        dact = dot(dy[...], wd[...], COLS_COLS).astype(BF16).astype(F32)
        sig = sigmoid(gate)
        silu = gate * sig
        act[...] = (silu * up).astype(BF16)
        by_up = (dact * silu).astype(BF16)
        by_gate = (dact * up * (sig + silu * (1.0 - sig))).astype(BF16)
        dgu[0] = by_gate
        dgu[1] = by_up
        if full:
            acc[...] += dot(by_gate, wg[...], COLS_COLS) + dot(by_up, wu[...], COLS_COLS)

            @pl.when(j == nc - 1)
            def _():
                dh[...] = by_normed(h[...], acc[...], dy[...])

        left()

    tile = pl.BlockSpec((T, D), lambda i, j: (i, 0))
    wide_tile = pl.BlockSpec((T, C), lambda i, j: (i, j))
    out = pl.pallas_call(
        kernel,
        grid=(nt, nc),
        out_shape=[jax.ShapeDtypeStruct((S, F), BF16), jax.ShapeDtypeStruct((2, S, F), BF16)]
        + [jax.ShapeDtypeStruct((S, D), BF16)] * (most - 2)
        + beside.outs,
        in_specs=[
            tile,
            tile,
            weight_spec((D, C), lambda i, j: (0, j), nc),
            weight_spec((D, C), lambda i, j: (0, j), nc),
            weight_spec((C, D), lambda i, j: (j, 0), nc),
        ]
        + [HBM] * len(beside.operands),
        out_specs=[wide_tile, pl.BlockSpec((2, T, C), lambda i, j: (0, i, j))] + [tile] * (most - 2) + beside.out_specs,
        scratch_shapes=[pltpu.VMEM((T, D), F32)] * full + beside.scratch,
        compiler_params=pltpu.CompilerParams(vmem_limit_bytes=LIMIT, dimension_semantics=("arbitrary", "arbitrary"), **beside.kind),
        cost_estimate=pl.CostEstimate(flops=10 * S * D * F, bytes_accessed=6 * S * F, transcendentals=S * F),
        name=f"backward{cid}",
    )(h, dy, wg, wu, wd, *beside.operands)
    return out[:most], out[most:]


def to_state(n, h, dy, dgu, wg, wu, terms, cid):
    S, D = h.shape
    F = wg.shape[1]
    T, C = cut(S, TILE["s_t"]), cut(F, TILE["s_c"])
    nt, nc = S // T, F // C
    steps = nt * nc
    beside = Beside(n, terms, TILE["s_when"], cid)

    def kernel(h, dy, dgu, wg, wu, *rest):
        k = len(beside.operands)
        terms_, dh, rest = rest[:k], rest[k], rest[k + 1 :]
        k = len(beside.outs)
        sums, acc, rest = rest[:k], rest[k], rest[k + 1 :]
        j = pl.program_id(1)
        step = pl.program_id(0) * nc + j
        left = beside.start(step, steps, terms_, sums, rest)

        @pl.when(j == 0)
        def _():
            acc[...] = jnp.zeros_like(acc)

        acc[...] += dot(dgu[0], wg[...], COLS_COLS) + dot(dgu[1], wu[...], COLS_COLS)

        @pl.when(j == nc - 1)
        def _():
            dh[...] = by_normed(h[...], acc[...], dy[...])

        left()

    tile = pl.BlockSpec((T, D), lambda i, j: (i, 0))
    wide_tile = pl.BlockSpec((2, T, C), lambda i, j: (0, i, j))
    weight = weight_spec((D, C), lambda i, j: (0, j), nc)
    out = pl.pallas_call(
        kernel,
        grid=(nt, nc),
        out_shape=[jax.ShapeDtypeStruct((S, D), BF16)] + beside.outs,
        in_specs=[tile, tile, wide_tile, weight, weight] + [HBM] * len(beside.operands),
        out_specs=[tile] + beside.out_specs,
        scratch_shapes=[pltpu.VMEM((T, D), F32)] + beside.scratch,
        compiler_params=pltpu.CompilerParams(vmem_limit_bytes=LIMIT, dimension_semantics=("arbitrary", "arbitrary"), **beside.kind),
        cost_estimate=pl.CostEstimate(flops=4 * S * D * F, bytes_accessed=4 * S * F, transcendentals=0),
        name="to_state",
    )(h, dy, dgu, wg, wu, *beside.operands)
    return out[0], out[1:]


def down_weight(act, dy):
    S, D = dy.shape
    F = act.shape[1]
    C = cut(F, TILE["d_c"])

    def kernel(act, dy, od):
        od[...] = dot(act[...], dy[...], ROWS_ROWS).astype(BF16)

    return pl.pallas_call(
        kernel,
        grid=(F // C,),
        out_shape=jax.ShapeDtypeStruct((F, D), BF16),
        in_specs=[pl.BlockSpec((S, C), lambda i: (0, i)), once((S, D), lambda i: (0, 0))],
        out_specs=pl.BlockSpec((C, D), lambda i: (i, 0)),
        compiler_params=pltpu.CompilerParams(vmem_limit_bytes=LIMIT, dimension_semantics=("arbitrary",)),
        cost_estimate=pl.CostEstimate(flops=2 * S * D * F, bytes_accessed=2 * S * F, transcendentals=0),
        name="down_weight",
    )(act, dy)


def gate_weights(n, a, dgu, terms, cid):
    S, D = a.shape
    F = dgu.shape[2]
    C = cut(F, TILE["g_c"])
    nc = F // C
    steps = 2 * nc
    beside = Beside(n, terms, TILE["g_when"], cid)

    def kernel(a, dgu, *rest):
        k = len(beside.operands)
        terms_, o, rest = rest[:k], rest[k], rest[k + 1 :]
        k = len(beside.outs)
        sums, rest = rest[:k], rest[k:]
        step = pl.program_id(0) * nc + pl.program_id(1)
        left = beside.start(step, steps, terms_, sums, rest)
        o[...] = dot(a[...], dgu[...], ROWS_ROWS).astype(BF16)
        left()

    out = pl.pallas_call(
        kernel,
        grid=(2, nc),
        out_shape=[jax.ShapeDtypeStruct((2, D, F), BF16)] + beside.outs,
        in_specs=[once((S, D), lambda k, j: (0, 0)), pl.BlockSpec((None, S, C), lambda k, j: (k, 0, j))] + [HBM] * len(beside.operands),
        out_specs=[pl.BlockSpec((None, D, C), lambda k, j: (k, 0, j))] + beside.out_specs,
        scratch_shapes=beside.scratch,
        compiler_params=pltpu.CompilerParams(vmem_limit_bytes=LIMIT, dimension_semantics=("arbitrary", "arbitrary"), **beside.kind),
        cost_estimate=pl.CostEstimate(flops=4 * S * D * F, bytes_accessed=4 * S * F, transcendentals=0),
        name=f"gate_weights{cid}",
    )(a, dgu, *beside.operands)
    return out[0], out[1:]


def solution(mesh):
    n = mesh.shape["dp"]

    def device(x, dy, wg, wu, wd):
        x, dy = x.reshape(x.shape[1:]), dy.reshape(dy.shape[1:])
        first, nexts = gather(n, wg, wu, wd, 0)
        w0 = whole(n, first)
        h, second = forward(n, x, *w0, nexts, 1)
        w1 = whole(n, second)

        (act, dgu, a, dh), _ = backward(n, h, dy, *w1, True, None, 2)
        down = down_weight(act, dy)
        gates, (down1,) = gate_weights(n, a, dgu, down, 3)

        (act, dgu, a), gates1 = backward(n, x, dh, *w0, False, gates, 4)
        down = down_weight(act, dh)
        gates, (down0,) = gate_weights(n, a, dgu, down, 5)
        dx, gates0 = to_state(n, x, dh, dgu, *w0[:2], gates, 6)
        sums = [(*gates0, down0), (*gates1, down1)]
        return (dx[None], *(jnp.stack([s[j] for s in sums]) for j in range(3)))

    tokens, rows = P(("rep", "dp")), P(None, "dp")
    return jax.shard_map(
        device, mesh=mesh, in_specs=(tokens, tokens, rows, rows, rows), out_specs=(tokens, *[P("rep", "dp")] * 3), check_vma=False
    )
```
